32 devices in a mesh: dp: 4 (over x, core), ctx: 8 (over z, y).
Axes of the slice: x: 2, y: 2, z: 4, core: 2. Of those that a mesh axis runs over, the one named last changes fastest.
Arguments:
- tokens: bfloat16 [4096, 1792], P(('dp', 'ctx')), may hold values from -6 to 6
- cotangent: bfloat16 [4096, 1792], P(('dp', 'ctx')), may hold values from -6 to 6
- expert_ids: int32 [4096, 4], P(('dp', 'ctx')), may hold values from 0 to 15, all different within a row; in each aligned block of 128 rows (0 to 127, 128 to 255, ...) at most 40 rows name the same one
- norm_gain: float32 [1792], replicated, may hold values from 0.5 to 1.5
- router_weight: bfloat16 [1792, 16], replicated, may hold values from -0.125 to 0.125
- gate_weight: bfloat16 [16, 1792, 1536], P('ctx', None, 'dp'), may hold values from -0.125 to 0.125
- up_weight: bfloat16 [16, 1792, 1536], P('ctx', None, 'dp'), may hold values from -0.125 to 0.125
- down_weight: bfloat16 [16, 1536, 1792], P('ctx', 'dp'), may hold values from -0.15625 to 0.15625
Outputs:
- grad_tokens: bfloat16 [4096, 1792], P(('dp', 'ctx'))
- grad_gate: bfloat16 [16, 1792, 1536], P('ctx', None, 'dp')
- grad_up: bfloat16 [16, 1792, 1536], P('ctx', None, 'dp')
- grad_down: bfloat16 [16, 1536, 1792], P('ctx', 'dp')
- grad_router: float32 [1792, 16], P(('dp', 'ctx'))
- grad_gain: float32 [1792], P(('dp', 'ctx'))
The draws below stay inside these ranges and needn't reach their ends.
Inputs may be any that keep to these rules, and one draw needn't show every extreme that they name: `expert_ids`: each row names 4 different experts; among the rows of one device no expert is named more than 40 times.
All inputs are finite; a program needn't handle non-finite values.
Results may differ from the reference program's by a relative error of at most 0.02.
Values may be sent and summed in bfloat16 or wider, within the bound.
A program may use at most 192 MiB of HBM per device.

```python
import math
import jax
import jax.numpy as jnp
import numpy as np
from jax import lax

D = 1792
FF = 1536
TOP = 4
TOK_DEV = 128
EXPERTS = 16
CAP = 40
TOKENS = 4096
N_DP = 4
N_CTX = 8


def raised(values, own_key, source, target, blocks, factor):
    def block_of(dim):
        return (jnp.arange(values.shape[dim]) // (values.shape[dim] // blocks)).reshape((-1,) + (1,) * (values.ndim - 1 - dim))

    near = jax.random.permutation(own_key, blocks)[block_of(target)]
    second = (block_of(target) + blocks // 2) % blocks
    return jnp.where((block_of(source) == near) | (block_of(source) == second), factor * values, values)


def block_scale(stream_key, shape, cuts, smallest, largest):
    gain, own = 1.0, jax.random.fold_in(stream_key, 6)
    for axis_at, shards_of in cuts:
        draws = jnp.exp(jax.random.uniform(jax.random.fold_in(own, axis_at), (shards_of,), jnp.float32, smallest / len(cuts), largest / len(cuts)))
        gain = gain * jnp.repeat(draws, shape[axis_at] // shards_of).reshape([-1 if axis == axis_at else 1 for axis in range(len(shape))])
    return gain


def shared_out(key, own, number, rows, count, top, bound, skew):
    order = jax.random.permutation(key, count)
    crowded, common = load_shares(count, rows * top, bound, skew, True), load_shares(count, rows * top, bound, skew, False)
    places = jnp.arange(count)

    def named(lengths, rotation):
        used = int((lengths > 0).sum())
        fixed = max(1, used // 4)
        moved = fixed + (places - fixed + rotation * (used - fixed)) % max(1, count - fixed)
        return jnp.zeros((count,), jnp.int32).at[order[jnp.where(places < fixed, places, moved)]].set(jnp.asarray(lengths, jnp.int32))

    lengths = jnp.where(number % 4 == 0, named(crowded, number // 4), named(common, number - number // 4 - 1))
    mixed = jax.random.permutation(jax.random.fold_in(own, 3), count)
    donor, taker = mixed[0:count // 2 * 2:2], mixed[1:count // 2 * 2:2]
    room = jnp.minimum(lengths[donor] - 1, bound - lengths[taker]) // 2
    room = jnp.where((donor == order[0]) | (taker == order[0]) | (lengths[taker] == 0), 0, jnp.maximum(room, 0))
    moved = jax.random.randint(jax.random.fold_in(own, 4), (count // 2,), 0, 1 << 20) % (room + 1)
    lengths = lengths.at[donor].add(-moved).at[taker].add(moved)
    items = jnp.searchsorted(jnp.cumsum(lengths), jnp.arange(rows * top), side="right").astype(jnp.int32)
    table = items.reshape(top, rows).T
    table = table[jax.random.permutation(jax.random.fold_in(own, 1), rows)]
    rotation = jax.random.randint(jax.random.fold_in(own, 2), (rows, 1), 0, top)
    return jnp.take_along_axis(table, (jnp.arange(top)[None, :] + rotation) % top, axis=1)


def load_shares(number_of, total, limit, lean, full):
    portions = [(1 << 20) // math.isqrt(rank ** lean) + 1 for rank in range(1, number_of + 1)]
    largest = limit if full else min(limit, max(-(-total // number_of), total * portions[0] // sum(portions)))
    least = 1 if total - largest >= number_of - 1 else 0
    counts, spare = [largest] + [least] * (number_of - 1), total - largest - least * (number_of - 1)
    while spare > 0:
        free = [i for i in range(1, number_of) if counts[i] < largest] or [i for i in range(1, number_of) if counts[i] < limit]
        pool, budget = sum([portions[i] for i in free]), spare
        for i in free:
            extra = min(limit - counts[i], max(1, budget * portions[i] // pool), spare)
            counts[i] = counts[i] + extra
            spare = spare - extra
    return np.array(counts)


def bell_draw(own_key, shape, width, most, pieces=(), held_as=jnp.bfloat16):
    gain = block_scale(own_key, shape, pieces, -0.22, 0.18) if pieces else 1.0
    result = jax.random.normal(own_key, shape, jnp.float32) * width * gain
    return jnp.minimum(jnp.maximum(result, -most), most).astype(held_as)


def gaussian_with(stream_key, shape, spread, limit, pieces, heavy, kind=jnp.bfloat16):
    values = spread * jax.random.normal(stream_key, shape, jnp.float32)
    if pieces:
        values = values * block_scale(stream_key, shape, pieces, -0.22, 0.18)
    return jnp.clip(raised(values, jax.random.fold_in(stream_key, 3), *heavy), -limit, limit).astype(kind)


def setup_inputs(seed: int = 0) -> dict:
    keys = jax.random.split(jax.random.key(seed), 9)
    tokens = gaussian_with(keys[0], (TOKENS, D), 1.0, 6.0, ((0, 32),), (0, 1, 32, 2.75))
    cotangent = bell_draw(keys[1], (TOKENS, D), 1.0, 6.0, ((0, 32),))
    expert_ids_keys = jax.random.split(jax.random.fold_in(keys[2], 1), TOKENS // TOK_DEV)
    expert_ids_turns = jax.random.permutation(jax.random.fold_in(keys[2], 3), TOKENS // TOK_DEV)
    expert_ids = jax.vmap(lambda own, number: shared_out(jax.random.fold_in(keys[2], 2), own, number, TOK_DEV, EXPERTS, TOP, CAP, 2))(expert_ids_keys, expert_ids_turns).reshape((TOKENS, TOP))
    norm_gain = jnp.clip(1.0 + 0.1 * jax.random.normal(keys[3], (D,), jnp.float32), 0.5, 1.5)
    router_weight = bell_draw(keys[4], (D, EXPERTS), D ** -0.5, 0.125)
    gate_weight = bell_draw(keys[5], (EXPERTS, D, FF), D ** -0.5, 0.125, ((0, 8), (2, 4)))
    up_weight = bell_draw(keys[6], (EXPERTS, D, FF), D ** -0.5, 0.125, ((0, 8), (2, 4)))
    down_weight = bell_draw(keys[7], (EXPERTS, FF, D), FF ** -0.5, 0.15625, ((0, 8), (1, 4)))
    return dict(tokens=tokens, cotangent=cotangent, expert_ids=expert_ids, norm_gain=norm_gain, router_weight=router_weight, gate_weight=gate_weight, up_weight=up_weight, down_weight=down_weight)


EPSILON = 1e-05
SWISH_SCALE = 1.702

def reference(tokens, cotangent, expert_ids, norm_gain, router_weight, gate_weight, up_weight, down_weight):
    ntoken = tokens.shape[0]
    widened = tokens.astype(jnp.float32)
    inverse = lax.rsqrt(lax.optimization_barrier(jnp.mean(widened * widened, axis=1, keepdims=True)) + EPSILON)
    scaled = widened * inverse
    normed = (scaled * norm_gain).astype(jnp.bfloat16)
    logits = jnp.dot(normed, router_weight, preferred_element_type=jnp.float32)
    chosen = jnp.take_along_axis(logits, expert_ids, axis=1)
    lifted = jnp.exp(chosen)
    gates = lifted / lax.optimization_barrier(jnp.sum(lifted, axis=1, keepdims=True))
    devices = N_DP * N_CTX
    per_device = TOK_DEV * TOP
    block_ids = expert_ids.reshape(devices, per_device)
    labels = jnp.arange(EXPERTS, dtype=jnp.int32)
    hits = (block_ids[:, :, None] == labels).astype(jnp.int32)
    rank = lax.optimization_barrier(jnp.sum((jnp.cumsum(hits, axis=1) - 1) * hits, axis=2))
    position = jnp.arange(devices, dtype=jnp.int32)[:, None] * CAP + rank
    assign = jnp.arange(devices * per_device, dtype=jnp.int32)
    flat_ids = block_ids.reshape(-1)
    flat_pos = position.reshape(-1).astype(jnp.int32)
    table = jnp.zeros((EXPERTS, devices * CAP), jnp.int32).at[flat_ids, flat_pos].set(assign)
    present_all = jnp.zeros((EXPERTS, devices * CAP), jnp.float32).at[flat_ids, flat_pos].set(1.0)
    gates_flat = gates.reshape(-1)

    def expert_step(carry, inputs):
        grad_tok, score_acc = carry
        entry, present, w_gate, w_up, w_down = inputs
        token = entry // TOP
        keep = present[:, None] > 0.0
        rows = jnp.where(keep, normed[token], jnp.zeros_like(normed[token]))
        upstream = jnp.where(keep, cotangent[token], jnp.zeros_like(cotangent[token]))
        weight = present * gates_flat[entry]
        gate_pre = jnp.dot(rows, w_gate, preferred_element_type=jnp.float32)
        up_pre = jnp.dot(rows, w_up, preferred_element_type=jnp.float32)
        squash = jax.nn.sigmoid(SWISH_SCALE * gate_pre)
        hidden = (gate_pre * squash * (up_pre + 1.0)).astype(jnp.bfloat16)
        grad_out = jnp.dot(upstream, w_down.T, preferred_element_type=jnp.float32)
        score = lax.optimization_barrier(jnp.sum(grad_out * hidden.astype(jnp.float32), axis=1))
        grad_hidden = weight[:, None] * grad_out
        slope = squash + SWISH_SCALE * gate_pre * squash * (1.0 - squash)
        grad_pre_gate = (grad_hidden * (up_pre + 1.0) * slope).astype(jnp.bfloat16)
        grad_pre_up = (grad_hidden * gate_pre * squash).astype(jnp.bfloat16)
        scaled_up = (weight[:, None] * upstream.astype(jnp.float32)).astype(jnp.bfloat16)
        down_grad = jnp.dot(hidden.T, scaled_up, preferred_element_type=jnp.float32).astype(jnp.bfloat16)
        gate_grad = jnp.dot(rows.T, grad_pre_gate, preferred_element_type=jnp.float32).astype(jnp.bfloat16)
        up_grad = jnp.dot(rows.T, grad_pre_up, preferred_element_type=jnp.float32).astype(jnp.bfloat16)
        back = jnp.dot(grad_pre_gate, w_gate.T, preferred_element_type=jnp.float32)
        back = back + jnp.dot(grad_pre_up, w_up.T, preferred_element_type=jnp.float32)
        grad_tok = grad_tok.at[token].add(back)
        score_acc = score_acc.at[entry].add(score * present)
        return ((grad_tok, score_acc), (gate_grad, up_grad, down_grad))
    start = (jnp.zeros((ntoken, D), jnp.float32), jnp.zeros((ntoken * TOP,), jnp.float32))
    (grad_tok, score_acc), (grad_gate, grad_up, grad_down) = lax.scan(expert_step, start, (table, present_all, gate_weight, up_weight, down_weight))
    score_tok = score_acc.reshape(ntoken, TOP)
    mixed = lax.optimization_barrier(jnp.sum(gates * score_tok, axis=1, keepdims=True))
    grad_chosen = gates * (score_tok - mixed)
    member = expert_ids[:, :, None] == labels
    grad_logits = lax.optimization_barrier(jnp.sum(jnp.where(member, grad_chosen[:, :, None], 0.0), axis=1)).astype(jnp.bfloat16)
    grad_normed = grad_tok + jnp.dot(grad_logits, router_weight.T, preferred_element_type=jnp.float32)
    grad_router = jnp.dot(normed.T, grad_logits, preferred_element_type=jnp.float32)
    grad_gain = lax.optimization_barrier(jnp.sum(grad_normed * scaled, axis=0))
    grad_scaled = grad_normed * norm_gain
    correction = lax.optimization_barrier(jnp.mean(grad_scaled * scaled, axis=1, keepdims=True))
    grad_tokens = (cotangent.astype(jnp.float32) + inverse * (grad_scaled - scaled * correction)).astype(jnp.bfloat16)
    return (grad_tokens, grad_gate, grad_up, grad_down, grad_router, grad_gain)
```

```python
import functools

import jax
import jax.numpy as jnp
from jax import lax
from jax.experimental import pallas as pl
from jax.experimental.pallas import tpu as pltpu
from jax.sharding import PartitionSpec as P

EPSILON = 1e-05
SWISH_SCALE = 1.702
INNER = 2
MESH = pl.DeviceIdType.MESH
ANY = pl.BlockSpec(memory_space=pl.ANY)
VMEM = pl.BlockSpec(memory_space=pltpu.VMEM)


def greet_all(n_dp, n_ctx):
    n = n_dp * n_ctx
    me = lax.axis_index("dp") * n_ctx + lax.axis_index("ctx")
    barrier = pltpu.get_barrier_semaphore()

    def hello(i, carry):
        peer = lax.rem(me + i, n)
        pl.semaphore_signal(
            barrier,
            inc=1,
            device_id=(lax.div(peer, n_ctx), lax.rem(peer, n_ctx)),
            device_id_type=MESH,
        )
        return carry

    lax.fori_loop(1, n, hello, 0)
    pl.semaphore_wait(barrier, n - 1)


def spread_copy(n_dp, n_ctx, i, src_of, land, send_sem, recv_sem, sending):
    n = n_dp * n_ctx
    me = lax.axis_index("dp") * n_ctx + lax.axis_index("ctx")
    peer = lax.rem(me + i, n)
    source = me if sending else lax.rem(me + n - i, n)
    return pltpu.make_async_remote_copy(
        src_ref=src_of(peer),
        dst_ref=land.at[source],
        send_sem=send_sem.at[i],
        recv_sem=recv_sem.at[i],
        device_id=(lax.div(peer, n_ctx), lax.rem(peer, n_ctx)),
        device_id_type=MESH,
    )


def exchange_kernel(n_dp, n_ctx, keep, x_ref, o_ref, land, send_sem, recv_sem):
    n = n_dp * n_ctx
    me = lax.axis_index("dp") * n_ctx + lax.axis_index("ctx")
    greet_all(n_dp, n_ctx)
    src_of = lambda peer: x_ref.at[peer]

    def start(i, carry):
        spread_copy(n_dp, n_ctx, i, src_of, land, send_sem, recv_sem, True).start()
        return carry

    lax.fori_loop(1, n, start, 0)
    land[pl.ds(me, 1)] = x_ref[pl.ds(me, 1)]

    def finish(i, carry):
        spread_copy(n_dp, n_ctx, i, src_of, land, send_sem, recv_sem, True).wait_send()
        spread_copy(n_dp, n_ctx, i, src_of, land, send_sem, recv_sem, False).wait_recv()
        return carry

    lax.fori_loop(1, n, finish, 0)
    o_ref[...] = jnp.sum(land[...].reshape(n // keep, keep, 8, 128), axis=0)


def exchange(x, n_dp, n_ctx, keep, cid):
    n = n_dp * n_ctx
    return pl.pallas_call(
        functools.partial(exchange_kernel, n_dp, n_ctx, keep),
        out_shape=jax.ShapeDtypeStruct((keep, 8, 128), jnp.float32),
        in_specs=[VMEM],
        out_specs=VMEM,
        scratch_shapes=[
            pltpu.VMEM((n, 8, 128), jnp.float32),
            pltpu.SemaphoreType.DMA((n,)),
            pltpu.SemaphoreType.DMA((n,)),
        ],
        compiler_params=pltpu.CompilerParams(collective_id=cid, has_side_effects=True),
    )(x)


def line_of(c, n_ctx):
    return lax.div(c, INNER), lax.rem(c, INNER), n_ctx // INNER


def line_step(z, length, q):
    near = jnp.minimum(z, length - 1 - z)
    around = z + lax.div(q + 1, 2) * (1 - 2 * lax.rem(q, 2))
    beyond = jnp.where(z < length - 1 - z, q, length - 1 - q)
    return jnp.where(q <= 2 * near, around, beyond)


def slot_masks(meta, picks, cap, base):
    places = (lax.broadcasted_iota(jnp.int32, (cap, meta.shape[1]), 0) + base).astype(jnp.float32)
    return [meta[k : k + 1] == places for k in range(picks)]


def dispatch_kernel(
    n_dp, n_ctx, cap, rows_ref, grad_ref, meta_ref, wg_ref, wu_ref, wd_ref,
    out_rows, out_grad, out_pair, out_hid, out_back, out_score,
    dense, meta_all, sel_own, sel_side, pair_w, down_w, chunk, pair_out, hid_out, back_out,
    meta_send, meta_recv, own_sem, weight_sem, line_send, line_recv, side_send, side_recv,
    far_send, far_recv, sib_send, sib_recv, store_sem, chunk_sem, result_sem,
):
    n = n_dp * n_ctx
    local, depth = wd_ref.shape[0], wd_ref.shape[1]
    picks = meta_ref.shape[1] // 2
    d, c = lax.axis_index("dp"), lax.axis_index("ctx")
    z, y, length = line_of(c, n_ctx)
    me = d * n_ctx + c
    side = z * INNER + 1 - y
    far = lax.rem(d + 2, n_dp)
    sib = d + 1 - 2 * lax.rem(d, 2)
    far_sib = lax.rem(sib + 2, n_dp)
    ins, outs = (rows_ref, grad_ref), (out_rows, out_grad)
    span = INNER * cap
    greet_all(n_dp, n_ctx)
    meta_src = lambda peer: meta_ref.at[0]

    def line_copy(a, j, up, first):
        return pltpu.make_async_remote_copy(
            src_ref=ins[a] if first else dense.at[a, j],
            dst_ref=dense.at[a, j],
            send_sem=line_send.at[a, int(up), j],
            recv_sem=line_recv.at[a, j],
            device_id=(d, (z + (1 if up else -1)) * INNER + y),
            device_id_type=MESH,
        )

    def relay(a, j, first, act):
        @pl.when((j <= z) & (z < length - 1))
        def _():
            act(line_copy(a, j, True, first))

        @pl.when((j >= z) & (z > 0))
        def _():
            act(line_copy(a, j, False, first))

    def meta_start(i, carry):
        spread_copy(n_dp, n_ctx, i, meta_src, meta_all, meta_send, meta_recv, True).start()
        return carry

    for a in range(2):
        relay(a, z, True, lambda copy: copy.start())
    lax.fori_loop(1, n, meta_start, 0)
    meta_all[pl.ds(me, 1)] = meta_ref[...]
    loads = [pltpu.make_async_copy(ins[a], dense.at[a, z], own_sem.at[a]) for a in range(2)]
    for load in loads:
        load.start()
    wloads = (
        pltpu.make_async_copy(wg_ref, pair_w.at[:, :, pl.ds(0, depth)], weight_sem.at[0]),
        pltpu.make_async_copy(wu_ref, pair_w.at[:, :, pl.ds(depth, depth)], weight_sem.at[1]),
        pltpu.make_async_copy(wd_ref, down_w, weight_sem.at[2]),
    )
    for load in wloads:
        load.start()

    def place(a, row, owner):
        slot = row * n_ctx + owner
        return outs[a].at[:, pl.ds(pl.multiple_of(slot * cap, 8), cap)]

    def forward(a, src, row, owner, to, send_sem, recv_sem):
        return pltpu.make_async_remote_copy(
            src_ref=src,
            dst_ref=place(a, row, owner),
            send_sem=send_sem,
            recv_sem=recv_sem,
            device_id=(to, c),
            device_id_type=MESH,
        )

    def near_copies(a, src, owner):
        return (
            forward(a, src, d, owner, far, far_send.at[a, owner], far_recv.at[a, owner]),
            forward(a, src, d, owner, sib, sib_send.at[a, 0, owner], sib_recv.at[a, 0, owner]),
        )

    def sib_copy(a, owner):
        src = place(a, far, owner)
        return forward(a, src, far, owner, sib, sib_send.at[a, 1, owner], sib_recv.at[a, 1, owner])

    def await_far(a, owner):
        row = place(a, far, owner)
        forward(a, row, far, owner, far, far_send.at[a, owner], far_recv.at[a, owner]).wait_recv()

    def await_sib(a, which, row, owner):
        src = place(a, row, owner)
        forward(
            a, src, row, owner, sib, sib_send.at[a, which, owner], sib_recv.at[a, which, owner]
        ).wait_recv()

    def side_copy(a, j, sending):
        return pltpu.make_async_remote_copy(
            src_ref=sel_side.at[a, j],
            dst_ref=place(a, d, j * INNER + (y if sending else 1 - y)),
            send_sem=side_send.at[a, j],
            recv_sem=side_recv.at[a, j],
            device_id=(d, side),
            device_id_type=MESH,
        )

    def own_store(a, j):
        return pltpu.make_async_copy(
            sel_own.at[a, j], place(a, d, j * INNER + y), store_sem.at[a, j]
        )

    def select(a, j):
        meta = meta_all[d * n_ctx + j * INNER + y]
        held = dense[a, j]
        for target, owner in ((sel_own, c), (sel_side, side)):
            for e in range(local):
                masks = slot_masks(meta, picks, cap, (owner * local + e) * cap)
                pick = sum(jnp.where(mask, 1.0, 0.0) for mask in masks).astype(jnp.bfloat16)
                target[a, j, e] = jnp.dot(
                    pick, held, preferred_element_type=jnp.float32
                ).astype(jnp.bfloat16)

    def emit(a, j):
        select(a, j)
        side_copy(a, j, True).start()
        owner = j * INNER + y
        for copy in near_copies(a, sel_own.at[a, j], owner):
            copy.start()
        own_store(a, j).start()

    def take_side(a, j):
        side_copy(a, j, False).wait_recv()
        owner = j * INNER + 1 - y
        for copy in near_copies(a, place(a, d, owner), owner):
            copy.start()

    def meta_wait(src):
        i = lax.rem(me + n - src, n)
        spread_copy(n_dp, n_ctx, i, meta_src, meta_all, meta_send, meta_recv, False).wait_recv()

    def segment(row, j):
        return pl.ds(pl.multiple_of((row * n_ctx + j * INNER) * cap, 8), span)

    def chunk_loads(rows, j):
        return [
            pltpu.make_async_copy(
                outs[a].at[:, segment(row, j)],
                chunk.at[a, :, pl.ds(i * span, span)],
                chunk_sem.at[a, i],
            )
            for a in range(2)
            for i, row in enumerate(rows)
        ]

    def chunk_stores(rows, j):
        return [
            pltpu.make_async_copy(
                held.at[:, pl.ds(i * span, span)], out.at[:, segment(row, j)], result_sem.at[b, i]
            )
            for b, (held, out) in enumerate(
                ((pair_out, out_pair), (hid_out, out_hid), (back_out, out_back))
            )
            for i, row in enumerate(rows)
        ]

    def compute(rows, j):
        for copy in chunk_loads(rows, j):
            copy.start()
        for copy in chunk_loads(rows, j):
            copy.wait()
        sources = [row * n_ctx + j * INNER + side_at for row in rows for side_at in range(INNER)]

        def expert(e, carry):
            masks = [
                slot_masks(meta_all[src], picks, cap, (c * local + e) * cap) for src in sources
            ]
            weight = jnp.concatenate(
                [
                    jnp.sum(
                        sum(
                            jnp.where(mask, meta_all[src, picks + k][None, :], 0.0)
                            for k, mask in enumerate(block)
                        ),
                        axis=1,
                        keepdims=True,
                    )
                    for src, block in zip(sources, masks)
                ],
                axis=0,
            )
            pre = jnp.dot(chunk[0, e], pair_w[e], preferred_element_type=jnp.float32)
            grad_out = lax.dot_general(
                chunk[1, e], down_w[e], (((1,), (1,)), ((), ())),
                preferred_element_type=jnp.float32,
            )
            gate_pre, up_pre = pre[:, :depth], pre[:, depth:]
            squash = jax.nn.sigmoid(SWISH_SCALE * gate_pre)
            swish = gate_pre * squash
            raised = up_pre + 1.0
            full = swish * raised
            hid_out[e] = (weight * full).astype(jnp.bfloat16)
            score = jnp.sum(
                grad_out * full.astype(jnp.bfloat16).astype(jnp.float32), axis=1, keepdims=True
            )
            grad_hidden = weight * grad_out
            slope = squash + SWISH_SCALE * swish * (1.0 - squash)
            pair_out[e, :, pl.ds(0, depth)] = (grad_hidden * raised * slope).astype(jnp.bfloat16)
            pair_out[e, :, pl.ds(depth, depth)] = (grad_hidden * swish).astype(jnp.bfloat16)
            back_out[e] = lax.dot_general(
                pair_out[e], pair_w[e], (((1,), (1,)), ((), ())),
                preferred_element_type=jnp.float32,
            ).astype(jnp.bfloat16)
            for i, (src, block) in enumerate(zip(sources, masks)):
                part = score[i * cap : (i + 1) * cap]
                lines = [
                    jnp.sum(jnp.where(mask, part, 0.0), axis=0, keepdims=True) for mask in block
                ]
                lines.append(jnp.zeros((picks, lines[0].shape[1]), jnp.float32))
                out_score[src] = out_score[src] + jnp.concatenate(lines, axis=0)
            return carry

        lax.fori_loop(0, local, expert, 0)
        for copy in chunk_stores(rows, j):
            copy.start()

    out_score[...] = jnp.zeros_like(out_score)
    for load in loads:
        load.wait()
    for a in range(2):
        emit(a, z)
    for load in wloads:
        load.wait()

    def line_meta(i, carry):
        src = d * n_ctx + lax.rem(z + i, length) * INNER + y
        meta_wait(src)
        return carry

    lax.fori_loop(1, length, line_meta, 0)

    def first_half(q):
        j = line_step(z, length, q)
        for a in range(2):
            own_store(a, j).wait()
            for side_at in range(INNER):
                await_sib(a, 0, sib, j * INNER + side_at)

        @pl.when(q > 0)
        def _():
            for copy in chunk_stores((d, sib), line_step(z, length, q - 1)):
                copy.wait()

        compute((d, sib), j)

    def outward(q, carry):
        j, before = line_step(z, length, q), line_step(z, length, q - 1)
        for a in range(2):
            line_copy(a, j, True, False).wait_recv()
            relay(a, j, False, lambda copy: copy.start())
            emit(a, j)
            take_side(a, before)

        @pl.when(q == 1)
        def _():
            lax.fori_loop(1, n, other_meta, 0)

        first_half(q - 1)
        return carry

    def other_meta(i, carry):
        src = lax.rem(me + n - i, n)
        inside = (lax.div(src, n_ctx) == d) & (lax.rem(src, INNER) == y)

        @pl.when(jnp.logical_not(inside))
        def _():
            meta_wait(src)

        return carry

    lax.fori_loop(1, length, outward, 0)
    last = line_step(z, length, length - 1)
    for a in range(2):
        take_side(a, last)
    first_half(length - 1)

    def inward(q, carry):
        j = line_step(z, length, q)
        for a in range(2):
            for owner in (j * INNER + y, j * INNER + 1 - y):
                await_far(a, owner)
                sib_copy(a, owner).start()
        for a in range(2):
            for owner in (j * INNER + y, j * INNER + 1 - y):
                await_sib(a, 1, far_sib, owner)

        @pl.when(q == 0)
        def _():
            for copy in chunk_stores((d, sib), last):
                copy.wait()

        @pl.when(q > 0)
        def _():
            for copy in chunk_stores((far, far_sib), line_step(z, length, q - 1)):
                copy.wait()

        compute((far, far_sib), j)
        return carry

    lax.fori_loop(0, length, inward, 0)
    for a in range(2):
        relay(a, z, True, lambda copy: copy.wait_send())

    def drain(q, carry):
        j = line_step(z, length, q)
        for a in range(2):

            @pl.when(q > 0)
            def _(a=a):
                relay(a, j, False, lambda copy: copy.wait_send())

            side_copy(a, j, True).wait_send()
            for owner in (j * INNER + y, j * INNER + 1 - y):
                for copy in near_copies(a, place(a, d, owner), owner):
                    copy.wait_send()
                sib_copy(a, owner).wait_send()
        return carry

    lax.fori_loop(0, length, drain, 0)

    def meta_finish(i, carry):
        spread_copy(n_dp, n_ctx, i, meta_src, meta_all, meta_send, meta_recv, True).wait_send()
        return carry

    lax.fori_loop(1, n, meta_finish, 0)
    for copy in chunk_stores((far, far_sib), last):
        copy.wait()


def dispatch_rows(rows, grad, meta, gate_weight, up_weight, down_weight, cap, n_dp, n_ctx):
    n = n_dp * n_ctx
    length = n_ctx // INNER
    tokens, width = rows.shape
    local, _, hidden = gate_weight.shape
    low = rows.dtype
    span = 2 * INNER * cap
    arrived = jax.ShapeDtypeStruct((local, n * cap, width), low)
    dma = pltpu.SemaphoreType.DMA
    return pl.pallas_call(
        functools.partial(dispatch_kernel, n_dp, n_ctx, cap),
        out_shape=(
            arrived,
            arrived,
            jax.ShapeDtypeStruct((local, n * cap, 2 * hidden), low),
            jax.ShapeDtypeStruct((local, n * cap, hidden), low),
            arrived,
            jax.ShapeDtypeStruct((n,) + meta.shape[1:], jnp.float32),
        ),
        in_specs=[ANY, ANY, VMEM, ANY, ANY, ANY],
        out_specs=(ANY,) * 5 + (VMEM,),
        scratch_shapes=[
            pltpu.VMEM((2, length, tokens, width), low),
            pltpu.VMEM((n,) + meta.shape[1:], jnp.float32),
            pltpu.VMEM((2, length, local, cap, width), low),
            pltpu.VMEM((2, length, local, cap, width), low),
            pltpu.VMEM((local, width, 2 * hidden), low),
            pltpu.VMEM(down_weight.shape, low),
            pltpu.VMEM((2, local, span, width), low),
            pltpu.VMEM((local, span, 2 * hidden), low),
            pltpu.VMEM((local, span, hidden), low),
            pltpu.VMEM((local, span, width), low),
            dma((n,)),
            dma((n,)),
            dma((2,)),
            dma((3,)),
            dma((2, 2, length)),
            dma((2, length)),
            dma((2, length)),
            dma((2, length)),
            dma((2, n_ctx)),
            dma((2, n_ctx)),
            dma((2, 2, n_ctx)),
            dma((2, 2, n_ctx)),
            dma((2, length)),
            dma((2, 2)),
            dma((3, 2)),
        ],
        compiler_params=pltpu.CompilerParams(
            collective_id=0, has_side_effects=True, vmem_limit_bytes=60 * 1024 * 1024
        ),
    )(rows, grad, meta, gate_weight, up_weight, down_weight)


def return_kernel(
    n_dp, n_ctx, cap, tile, back_ref, rows_ref, grad_ref, pair_ref, hid_ref, score_ref,
    out_ref, gate_out, up_out, down_out, out_score,
    mine, sib_land, far_out, far_land, done, pair, hid_raw, hid, row_tile, grad_tile, both, down,
    mine_sem, sib_send, sib_recv, far_send, far_recv, ring_send, ring_recv, own_sem,
    hold_sem, tile_sem, result_sem, score_send, score_recv,
):
    d, c = lax.axis_index("dp"), lax.axis_index("ctx")
    local = back_ref.shape[0]
    width, depth = rows_ref.shape[2], hid_ref.shape[2]
    across = width // tile
    units = local * across
    far = lax.rem(d + 2, n_dp)
    sib = d + 1 - 2 * lax.rem(d, 2)
    far_sib = lax.rem(sib + 2, n_dp)
    greet_all(n_dp, n_ctx)

    def dest(k):
        return lax.rem(c + k, n_ctx)

    def block(slot):
        return back_ref.at[:, pl.ds(pl.multiple_of(slot * cap, 8), cap)]

    def to_sib(k, which):
        row = far_sib if which == 0 else sib
        return pltpu.make_async_remote_copy(
            src_ref=block(row * n_ctx + dest(k)),
            dst_ref=sib_land.at[k, which],
            send_sem=sib_send.at[k, which],
            recv_sem=sib_recv.at[k, which],
            device_id=(sib, c),
            device_id_type=MESH,
        )

    def load(k, which):
        row = far if which == 0 else d
        return pltpu.make_async_copy(
            block(row * n_ctx + dest(k)), mine.at[k, which], mine_sem.at[k, which]
        )

    def to_far(k):
        return pltpu.make_async_remote_copy(
            src_ref=far_out.at[k],
            dst_ref=far_land.at[k],
            send_sem=far_send.at[k],
            recv_sem=far_recv.at[k],
            device_id=(far, c),
            device_id_type=MESH,
        )

    def ring(k, sending):
        owner = c if sending else lax.rem(c + n_ctx - k, n_ctx)
        return pltpu.make_async_remote_copy(
            src_ref=done.at[k],
            dst_ref=out_ref.at[owner],
            send_sem=ring_send.at[k],
            recv_sem=ring_recv.at[k],
            device_id=(d, dest(k)),
            device_id_type=MESH,
        )

    gaps = n_ctx + 1

    def turn(i):
        return lax.rem(i + 1, n_ctx)

    def tile_loads(u):
        e, slot = lax.div(u, across), lax.rem(u, 2)
        columns = pl.ds(pl.multiple_of(lax.rem(u, across) * tile, tile), tile)
        return (
            pltpu.make_async_copy(
                rows_ref.at[e, :, columns], row_tile.at[slot], tile_sem.at[0, slot]
            ),
            pltpu.make_async_copy(
                grad_ref.at[e, :, columns], grad_tile.at[slot], tile_sem.at[1, slot]
            ),
        )

    def results(u):
        e = lax.div(u, across)
        columns = pl.ds(pl.multiple_of(lax.rem(u, across) * tile, tile), tile)
        return (
            pltpu.make_async_copy(
                both.at[u, :, pl.ds(0, depth)], gate_out.at[e, columns], result_sem.at[0, u]
            ),
            pltpu.make_async_copy(
                both.at[u, :, pl.ds(depth, depth)], up_out.at[e, columns], result_sem.at[1, u]
            ),
            pltpu.make_async_copy(down.at[u], down_out.at[e, :, columns], result_sem.at[2, u]),
        )

    def unit(u, carry):
        for copy in tile_loads(u):
            copy.wait()

        @pl.when(u + 1 < units)
        def _():
            for copy in tile_loads(u + 1):
                copy.start()

        e, slot = lax.div(u, across), lax.rem(u, 2)
        both[u] = jnp.dot(
            row_tile[slot].T, pair[e], preferred_element_type=jnp.float32
        ).astype(jnp.bfloat16)
        down[u] = jnp.dot(
            hid[e], grad_tile[slot], preferred_element_type=jnp.float32
        ).astype(jnp.bfloat16)
        for copy in results(u):
            copy.start()
        return carry

    n = n_dp * n_ctx
    me = d * n_ctx + c
    score_src = lambda peer: score_ref.at[peer]

    def score_start(i, carry):
        spread_copy(n_dp, n_ctx, i, score_src, out_score, score_send, score_recv, True).start()
        return carry

    def score_finish(i, carry):
        spread_copy(n_dp, n_ctx, i, score_src, out_score, score_send, score_recv, True).wait_send()
        spread_copy(n_dp, n_ctx, i, score_src, out_score, score_send, score_recv, False).wait_recv()
        return carry

    def begin(i, carry):
        k = turn(i)
        for which in range(2):
            to_sib(k, which).start()
            load(k, which).start()
        return carry

    lax.fori_loop(0, n_ctx, begin, 0)
    holds = (
        pltpu.make_async_copy(pair_ref, pair, hold_sem.at[0]),
        pltpu.make_async_copy(hid_ref, hid_raw, hold_sem.at[1]),
    )
    for copy in holds:
        copy.start()
    for copy in tile_loads(0):
        copy.start()

    def outward(i, carry):
        k = turn(i)
        to_sib(k, 0).wait_recv()
        load(k, 0).wait()
        far_out[k] = (
            mine[k, 0].astype(jnp.float32) + sib_land[k, 0].astype(jnp.float32)
        ).astype(jnp.bfloat16)
        to_far(k).start()
        return carry

    lax.fori_loop(0, n_ctx, outward, 0)
    lax.fori_loop(1, n, score_start, 0)
    out_score[pl.ds(me, 1)] = score_ref[pl.ds(me, 1)]
    for copy in holds:
        copy.wait()
    for e in range(local):
        hid[e] = hid_raw[e].T

    def inward(i, carry):
        k = turn(i)
        lax.fori_loop(lax.div(i * units, gaps), lax.div((i + 1) * units, gaps), unit, 0)
        to_sib(k, 1).wait_recv()
        load(k, 1).wait()
        to_far(k).wait_recv()
        done[k] = (
            mine[k, 1].astype(jnp.float32)
            + sib_land[k, 1].astype(jnp.float32)
            + far_land[k].astype(jnp.float32)
        ).astype(jnp.bfloat16)

        @pl.when(k > 0)
        def _():
            ring(k, True).start()

        return carry

    lax.fori_loop(0, n_ctx, inward, 0)
    own = pltpu.make_async_copy(done.at[0], out_ref.at[c], own_sem)
    own.start()
    lax.fori_loop(n_ctx * units // gaps, units, unit, 0)
    own.wait()
    lax.fori_loop(1, n, score_finish, 0)

    def drain(k, carry):
        to_sib(k, 0).wait_send()
        to_sib(k, 1).wait_send()
        to_far(k).wait_send()

        @pl.when(k > 0)
        def _():
            ring(k, True).wait_send()
            ring(k, False).wait_recv()

        return carry

    lax.fori_loop(0, n_ctx, drain, 0)

    def store_wait(u, carry):
        for copy in results(u):
            copy.wait()
        return carry

    lax.fori_loop(0, units, store_wait, 0)


def return_rows(back, rows, grad, pair, hidden, score, n_dp, n_ctx):
    local, total, width = back.shape
    cap = total // (n_dp * n_ctx)
    depth = hidden.shape[2]
    tile = 256 if width % 256 == 0 else 128
    units = local * (width // tile)
    block = (local, cap, width)
    low = back.dtype
    return pl.pallas_call(
        functools.partial(return_kernel, n_dp, n_ctx, cap, tile),
        out_shape=(
            jax.ShapeDtypeStruct((n_ctx,) + block, low),
            jax.ShapeDtypeStruct((local, width, depth), low),
            jax.ShapeDtypeStruct((local, width, depth), low),
            jax.ShapeDtypeStruct((local, depth, width), low),
            jax.ShapeDtypeStruct(score.shape, jnp.float32),
        ),
        in_specs=[ANY] * 5 + [VMEM],
        out_specs=(ANY,) * 4 + (VMEM,),
        scratch_shapes=[
            pltpu.VMEM((n_ctx, 2) + block, low),
            pltpu.VMEM((n_ctx, 2) + block, low),
            pltpu.VMEM((n_ctx,) + block, low),
            pltpu.VMEM((n_ctx,) + block, low),
            pltpu.VMEM((n_ctx,) + block, low),
            pltpu.VMEM((local, total, 2 * depth), low),
            pltpu.VMEM((local, total, depth), low),
            pltpu.VMEM((local, depth, total), low),
            pltpu.VMEM((2, total, tile), low),
            pltpu.VMEM((2, total, tile), low),
            pltpu.VMEM((units, tile, 2 * depth), low),
            pltpu.VMEM((units, depth, tile), low),
            pltpu.SemaphoreType.DMA((n_ctx, 2)),
            pltpu.SemaphoreType.DMA((n_ctx, 2)),
            pltpu.SemaphoreType.DMA((n_ctx, 2)),
            pltpu.SemaphoreType.DMA((n_ctx,)),
            pltpu.SemaphoreType.DMA((n_ctx,)),
            pltpu.SemaphoreType.DMA((n_ctx,)),
            pltpu.SemaphoreType.DMA((n_ctx,)),
            pltpu.SemaphoreType.DMA,
            pltpu.SemaphoreType.DMA((2,)),
            pltpu.SemaphoreType.DMA((2, 2)),
            pltpu.SemaphoreType.DMA((3, units)),
            pltpu.SemaphoreType.DMA((n_dp * n_ctx,)),
            pltpu.SemaphoreType.DMA((n_dp * n_ctx,)),
        ],
        compiler_params=pltpu.CompilerParams(
            collective_id=1, has_side_effects=True, vmem_limit_bytes=60 * 1024 * 1024
        ),
    )(back, rows, grad, pair, hidden, score)


def tiles(x):
    return jnp.pad(x, ((0, 0), (0, 1024 - x.shape[1]))).reshape(x.shape[0], 8, 128)


def body(
    tokens, cotangent, expert_ids, norm_gain, router_weight, gate_weight, up_weight, down_weight
):
    n_ctx = lax.axis_size("ctx")
    n_dp = lax.axis_size("dp")
    n = n_dp * n_ctx
    local = gate_weight.shape[0]
    experts = router_weight.shape[1]
    rows_here = tokens.shape[0]
    picks = expert_ids.shape[1]
    width = tokens.shape[1]
    capacity = max(2, rows_here * picks * 5 // (4 * experts))
    capacity = -(-capacity // 8) * 8
    slots = experts * capacity
    widened = tokens.astype(jnp.float32)
    inverse = lax.rsqrt(jnp.mean(widened * widened, axis=1, keepdims=True) + EPSILON)
    scaled = widened * inverse
    normed = (scaled * norm_gain).astype(jnp.bfloat16)
    logits = jnp.dot(normed, router_weight, preferred_element_type=jnp.float32)
    labels = jnp.arange(experts, dtype=jnp.int32)
    member = expert_ids[:, :, None] == labels
    chosen = jnp.sum(jnp.where(member, logits[:, None, :], 0.0), axis=2)
    lifted = jnp.exp(chosen)
    gates = lifted / jnp.sum(lifted, axis=1, keepdims=True)
    hits = jnp.any(member, axis=1).astype(jnp.bfloat16)
    earlier = jnp.tril(jnp.ones((rows_here, rows_here), jnp.bfloat16), -1)
    count = jnp.dot(earlier, hits, preferred_element_type=jnp.float32)
    rank = jnp.sum(jnp.where(member, count[:, None, :], 0.0), axis=2)
    position = expert_ids.astype(jnp.float32) * capacity + rank
    meta = jnp.concatenate([position, gates], axis=1).T[None]
    rows, upstream, pair, hidden, back, score = dispatch_rows(
        normed, cotangent, meta, gate_weight, up_weight, down_weight, capacity, n_dp, n_ctx
    )
    back_slots, gate_grad, up_grad, down_grad, score_parts = return_rows(
        back, rows, upstream, pair, hidden, score, n_dp, n_ctx
    )
    score_tok = jnp.sum(score_parts, axis=0)[:picks].T
    back_flat = back_slots.reshape(slots, width)
    places = jnp.arange(slots, dtype=jnp.float32)[:, None]
    match = [places == position[:, k][None, :] for k in range(picks)]
    dispatch_low = sum(jnp.where(hit, 1.0, 0.0) for hit in match).astype(jnp.bfloat16)
    grad_tok = jnp.dot(dispatch_low.T, back_flat, preferred_element_type=jnp.float32)
    mixed = jnp.sum(gates * score_tok, axis=1, keepdims=True)
    grad_chosen = gates * (score_tok - mixed)
    grad_logits = jnp.sum(jnp.where(member, grad_chosen[:, :, None], 0.0), axis=1).astype(
        jnp.bfloat16
    )
    grad_normed = grad_tok + jnp.dot(
        grad_logits, router_weight.T, preferred_element_type=jnp.float32
    )
    router_part = jnp.dot(normed.T, grad_logits, preferred_element_type=jnp.float32)
    gain_part = jnp.sum(grad_normed * scaled, axis=0)
    share = width // n
    parts = jnp.concatenate(
        [router_part.reshape(n, share * experts), gain_part.reshape(n, share)], axis=1
    )
    sums = exchange(tiles(parts), n_dp, n_ctx, 1, 3).reshape(1024)
    router_grad = sums[: share * experts].reshape(share, experts)
    gain_grad = sums[share * experts : share * experts + share]
    grad_scaled = grad_normed * norm_gain
    correction = jnp.mean(grad_scaled * scaled, axis=1, keepdims=True)
    grad_input = (
        cotangent.astype(jnp.float32) + inverse * (grad_scaled - scaled * correction)
    ).astype(jnp.bfloat16)
    return (grad_input, gate_grad, up_grad, down_grad, router_grad, gain_grad)


def solution(mesh):
    return jax.shard_map(
        body,
        mesh=mesh,
        in_specs=(
            P(("dp", "ctx"), None),
            P(("dp", "ctx"), None),
            P(("dp", "ctx"), None),
            P(),
            P(),
            P("ctx", None, "dp"),
            P("ctx", None, "dp"),
            P("ctx", "dp", None),
        ),
        out_specs=(
            P(("dp", "ctx"), None),
            P("ctx", None, "dp"),
            P("ctx", None, "dp"),
            P("ctx", "dp", None),
            P(("dp", "ctx"), None),
            P(("dp", "ctx")),
        ),
        check_vma=False,
    )
```

```python
import functools

import jax
import jax.numpy as jnp
from jax import lax
from jax.experimental import pallas as pl
from jax.experimental.pallas import tpu as pltpu
from jax.sharding import PartitionSpec as P

EPSILON = 1e-05
SWISH_SCALE = 1.702
INNER = 2
MESH = pl.DeviceIdType.MESH
ANY = pl.BlockSpec(memory_space=pl.ANY)
VMEM = pl.BlockSpec(memory_space=pltpu.VMEM)


def greet_all(n_dp, n_ctx):
    n = n_dp * n_ctx
    me = lax.axis_index("dp") * n_ctx + lax.axis_index("ctx")
    barrier = pltpu.get_barrier_semaphore()

    def hello(i, carry):
        peer = lax.rem(me + i, n)
        pl.semaphore_signal(
            barrier,
            inc=1,
            device_id=(lax.div(peer, n_ctx), lax.rem(peer, n_ctx)),
            device_id_type=MESH,
        )
        return carry

    lax.fori_loop(1, n, hello, 0)
    pl.semaphore_wait(barrier, n - 1)


def spread_copy(n_dp, n_ctx, i, src_of, land, send_sem, recv_sem, sending):
    n = n_dp * n_ctx
    me = lax.axis_index("dp") * n_ctx + lax.axis_index("ctx")
    peer = lax.rem(me + i, n)
    source = me if sending else lax.rem(me + n - i, n)
    return pltpu.make_async_remote_copy(
        src_ref=src_of(peer),
        dst_ref=land.at[source],
        send_sem=send_sem.at[i],
        recv_sem=recv_sem.at[i],
        device_id=(lax.div(peer, n_ctx), lax.rem(peer, n_ctx)),
        device_id_type=MESH,
    )


def exchange_kernel(n_dp, n_ctx, keep, x_ref, o_ref, land, send_sem, recv_sem):
    n = n_dp * n_ctx
    me = lax.axis_index("dp") * n_ctx + lax.axis_index("ctx")
    greet_all(n_dp, n_ctx)
    src_of = lambda peer: x_ref.at[peer]

    def start(i, carry):
        spread_copy(n_dp, n_ctx, i, src_of, land, send_sem, recv_sem, True).start()
        return carry

    lax.fori_loop(1, n, start, 0)
    land[pl.ds(me, 1)] = x_ref[pl.ds(me, 1)]

    def finish(i, carry):
        spread_copy(n_dp, n_ctx, i, src_of, land, send_sem, recv_sem, True).wait_send()
        spread_copy(n_dp, n_ctx, i, src_of, land, send_sem, recv_sem, False).wait_recv()
        return carry

    lax.fori_loop(1, n, finish, 0)
    o_ref[...] = jnp.sum(land[...].reshape(n // keep, keep, 8, 128), axis=0)


def exchange(x, n_dp, n_ctx, keep, cid):
    n = n_dp * n_ctx
    return pl.pallas_call(
        functools.partial(exchange_kernel, n_dp, n_ctx, keep),
        out_shape=jax.ShapeDtypeStruct((keep, 8, 128), jnp.float32),
        in_specs=[VMEM],
        out_specs=VMEM,
        scratch_shapes=[
            pltpu.VMEM((n, 8, 128), jnp.float32),
            pltpu.SemaphoreType.DMA((n,)),
            pltpu.SemaphoreType.DMA((n,)),
        ],
        compiler_params=pltpu.CompilerParams(collective_id=cid, has_side_effects=True),
    )(x)


def line_of(c, n_ctx):
    return lax.div(c, INNER), lax.rem(c, INNER), n_ctx // INNER


def line_step(z, length, q):
    near = jnp.minimum(z, length - 1 - z)
    around = z + lax.div(q + 1, 2) * (1 - 2 * lax.rem(q, 2))
    beyond = jnp.where(z < length - 1 - z, q, length - 1 - q)
    return jnp.where(q <= 2 * near, around, beyond)


def slot_masks(meta, picks, cap, base):
    places = (lax.broadcasted_iota(jnp.int32, (cap, meta.shape[1]), 0) + base).astype(jnp.float32)
    return [meta[k : k + 1] == places for k in range(picks)]


def dispatch_kernel(
    n_dp, n_ctx, cap, rows_ref, grad_ref, meta_ref, wg_ref, wu_ref, wd_ref,
    out_rows, out_grad, out_pair, out_hid, out_back, out_score, meta_all,
    dense, sel_own, sel_side, pair_w, down_w, chunk, pair_out, hid_out, back_out,
    meta_send, meta_recv, own_sem, weight_sem, line_send, line_recv, side_send, side_recv,
    far_send, far_recv, sib_send, sib_recv, store_sem, chunk_sem, result_sem,
    cross_send, cross_recv,
):
    n = n_dp * n_ctx
    local, depth = wd_ref.shape[0], wd_ref.shape[1]
    picks = meta_ref.shape[1] // 2
    d, c = lax.axis_index("dp"), lax.axis_index("ctx")
    z, y, length = line_of(c, n_ctx)
    me = d * n_ctx + c
    side = z * INNER + 1 - y
    far = lax.rem(d + 2, n_dp)
    sib = d + 1 - 2 * lax.rem(d, 2)
    far_sib = lax.rem(sib + 2, n_dp)
    core = lax.rem(d, 2)
    streams = ((0, d, 0), (1, d, 0), (1, far, 1))
    ins, outs = (rows_ref, grad_ref), (out_rows, out_grad)
    span = INNER * cap
    greet_all(n_dp, n_ctx)
    meta_src = lambda peer: meta_ref.at[0]

    def line_copy(a, j, up, first):
        return pltpu.make_async_remote_copy(
            src_ref=ins[a] if first else dense.at[a, j],
            dst_ref=dense.at[a, j],
            send_sem=line_send.at[a, int(up), j],
            recv_sem=line_recv.at[a, j],
            device_id=(d, (z + (1 if up else -1)) * INNER + y),
            device_id_type=MESH,
        )

    def relay(a, j, first, act):
        @pl.when((j <= z) & (z < length - 1))
        def _():
            act(line_copy(a, j, True, first))

        @pl.when((j >= z) & (z > 0))
        def _():
            act(line_copy(a, j, False, first))

    def meta_start(i, carry):
        spread_copy(n_dp, n_ctx, i, meta_src, meta_all, meta_send, meta_recv, True).start()
        return carry

    def on_core(s, act):
        if s == 2:
            pl.when(core == 0)(act)
        else:
            act()

    cross = pltpu.make_async_remote_copy(
        src_ref=grad_ref,
        dst_ref=dense.at[2, z],
        send_sem=cross_send,
        recv_sem=cross_recv,
        device_id=(far, c),
        device_id_type=MESH,
    )
    lax.fori_loop(1, n, meta_start, 0)
    pl.when(core == 0)(lambda: cross.start())
    for a in range(2):
        relay(a, z, True, lambda copy: copy.start())
    meta_all[pl.ds(me, 1)] = meta_ref[...]
    loads = [pltpu.make_async_copy(ins[a], dense.at[a, z], own_sem.at[a]) for a in range(2)]
    for load in loads:
        load.start()
    wloads = (
        pltpu.make_async_copy(wg_ref, pair_w.at[:, :, pl.ds(0, depth)], weight_sem.at[0]),
        pltpu.make_async_copy(wu_ref, pair_w.at[:, :, pl.ds(depth, depth)], weight_sem.at[1]),
        pltpu.make_async_copy(wd_ref, down_w, weight_sem.at[2]),
    )
    for load in wloads:
        load.start()

    def place(a, row, owner):
        slot = row * n_ctx + owner
        return outs[a].at[:, pl.ds(pl.multiple_of(slot * cap, 8), cap)]

    def forward(a, src, row, owner, to, send_sem, recv_sem):
        return pltpu.make_async_remote_copy(
            src_ref=src,
            dst_ref=place(a, row, owner),
            send_sem=send_sem,
            recv_sem=recv_sem,
            device_id=(to, c),
            device_id_type=MESH,
        )

    def near_copies(s, src, owner, act):
        a, row, which = streams[s]
        to_far = lambda: act(
            forward(a, src, row, owner, far, far_send.at[a, owner], far_recv.at[a, owner])
        )
        if s == 0:
            to_far()
        if s == 1:
            pl.when(core == 1)(to_far)
        send, recv = sib_send.at[a, which, owner], sib_recv.at[a, which, owner]
        act(forward(a, src, row, owner, sib, send, recv))

    def sib_copy(a, owner):
        src = place(a, far, owner)
        return forward(a, src, far, owner, sib, sib_send.at[a, 1, owner], sib_recv.at[a, 1, owner])

    def await_far(a, owner):
        row = place(a, far, owner)
        forward(a, row, far, owner, far, far_send.at[a, owner], far_recv.at[a, owner]).wait_recv()

    def await_sib(a, which, row, owner):
        src = place(a, row, owner)
        forward(
            a, src, row, owner, sib, sib_send.at[a, which, owner], sib_recv.at[a, which, owner]
        ).wait_recv()

    def side_copy(s, j, sending):
        a, row, _ = streams[s]
        return pltpu.make_async_remote_copy(
            src_ref=sel_side.at[s, j],
            dst_ref=place(a, row, j * INNER + (y if sending else 1 - y)),
            send_sem=side_send.at[s, j],
            recv_sem=side_recv.at[s, j],
            device_id=(d, side),
            device_id_type=MESH,
        )

    def own_store(s, j):
        a, row, _ = streams[s]
        return pltpu.make_async_copy(
            sel_own.at[s, j], place(a, row, j * INNER + y), store_sem.at[s, j]
        )

    def select(s, j):
        meta = meta_all[streams[s][1] * n_ctx + j * INNER + y]
        held = dense[s, j]
        for target, owner in ((sel_own, c), (sel_side, side)):
            for e in range(local):
                masks = slot_masks(meta, picks, cap, (owner * local + e) * cap)
                pick = sum(jnp.where(mask, 1.0, 0.0) for mask in masks).astype(jnp.bfloat16)
                target[s, j, e] = jnp.dot(
                    pick, held, preferred_element_type=jnp.float32
                ).astype(jnp.bfloat16)

    def emit(s, j):
        select(s, j)
        side_copy(s, j, True).start()
        near_copies(s, sel_own.at[s, j], j * INNER + y, lambda copy: copy.start())
        own_store(s, j).start()

    def take_side(s, j):
        side_copy(s, j, False).wait_recv()
        a, row, _ = streams[s]
        owner = j * INNER + 1 - y
        near_copies(s, place(a, row, owner), owner, lambda copy: copy.start())

    def segment(row, j):
        return pl.ds(pl.multiple_of((row * n_ctx + j * INNER) * cap, 8), span)

    def chunk_loads(half, i, row, j):
        return [
            pltpu.make_async_copy(
                outs[a].at[:, segment(row, j)],
                chunk.at[half, a, :, pl.ds(i * span, span)],
                chunk_sem.at[half, a, i],
            )
            for a in range(2)
        ]

    def chunk_stores(half, rows, j):
        return [
            pltpu.make_async_copy(
                held.at[half, :, pl.ds(i * span, span)],
                out.at[:, segment(row, j)],
                result_sem.at[half, b, i],
            )
            for b, (held, out) in enumerate(
                ((pair_out, out_pair), (hid_out, out_hid), (back_out, out_back))
            )
            for i, row in enumerate(rows)
        ]

    def compute(half, rows, j):
        for i, row in enumerate(rows):
            for copy in chunk_loads(half, i, row, j):
                copy.wait()

        @pl.when(j != z)
        def _():
            for copy in chunk_stores(half, rows, j):
                copy.wait()

        sources = [row * n_ctx + j * INNER + side_at for row in rows for side_at in range(INNER)]

        def expert(e, carry):
            masks = [
                slot_masks(meta_all[src], picks, cap, (c * local + e) * cap) for src in sources
            ]
            weight = jnp.concatenate(
                [
                    jnp.sum(
                        sum(
                            jnp.where(mask, meta_all[src, picks + k][None, :], 0.0)
                            for k, mask in enumerate(block)
                        ),
                        axis=1,
                        keepdims=True,
                    )
                    for src, block in zip(sources, masks)
                ],
                axis=0,
            )
            pre = jnp.dot(chunk[half, 0, e], pair_w[e], preferred_element_type=jnp.float32)
            grad_out = lax.dot_general(
                chunk[half, 1, e], down_w[e], (((1,), (1,)), ((), ())),
                preferred_element_type=jnp.float32,
            )
            gate_pre, up_pre = pre[:, :depth], pre[:, depth:]
            squash = jax.nn.sigmoid(SWISH_SCALE * gate_pre)
            swish = gate_pre * squash
            raised = up_pre + 1.0
            full = swish * raised
            hid_out[half, e] = (weight * full).astype(jnp.bfloat16)
            score = jnp.sum(
                grad_out * full.astype(jnp.bfloat16).astype(jnp.float32), axis=1, keepdims=True
            )
            grad_hidden = weight * grad_out
            slope = squash + SWISH_SCALE * swish * (1.0 - squash)
            pair_out[half, e, :, pl.ds(0, depth)] = (grad_hidden * raised * slope).astype(jnp.bfloat16)
            pair_out[half, e, :, pl.ds(depth, depth)] = (grad_hidden * swish).astype(jnp.bfloat16)
            back_out[half, e] = lax.dot_general(
                pair_out[half, e], pair_w[e], (((1,), (1,)), ((), ())),
                preferred_element_type=jnp.float32,
            ).astype(jnp.bfloat16)
            for i, (src, block) in enumerate(zip(sources, masks)):
                part = score[i * cap : (i + 1) * cap]
                lines = [
                    jnp.sum(jnp.where(mask, part, 0.0), axis=0, keepdims=True) for mask in block
                ]
                lines.append(jnp.zeros((picks, lines[0].shape[1]), jnp.float32))
                out_score[src] = out_score[src] + jnp.concatenate(lines, axis=0)
            return carry

        lax.fori_loop(0, local, expert, 0)
        for copy in chunk_stores(half, rows, j):
            copy.start()

    out_score[...] = jnp.zeros_like(out_score)
    for load in loads:
        load.wait()
    for a in range(2):
        emit(a, z)
    for load in wloads:
        load.wait()

    def meta_arrival(i, carry):
        spread_copy(n_dp, n_ctx, i, meta_src, meta_all, meta_send, meta_recv, False).wait_recv()
        return carry

    lax.fori_loop(1, n, meta_arrival, 0)

    @pl.when(core == 0)
    def _():
        cross.wait_recv()
        relay(2, z, False, lambda copy: copy.start())
        emit(2, z)

    def each(r, act):
        def step(k, carry):
            j = z + (2 * k - 1) * r
            pl.when((j >= 0) & (j < length) & (r + k > 0))(lambda: act(j))
            return carry

        lax.fori_loop(0, 2, step, 0)

    def pass_far(j):
        def one(a):
            for owner in (j * INNER + y, j * INNER + 1 - y):
                await_far(a, owner)
                sib_copy(a, owner).start()

        one(0)
        pl.when(core == 1)(lambda: one(1))

    def first_half(j):
        for a in range(2):
            own_store(a, j).wait()
        for copy in chunk_loads(0, 0, d, j):
            copy.start()
        for a in range(2):
            for side_at in range(INNER):
                await_sib(a, 0, sib, j * INNER + side_at)
        for copy in chunk_loads(0, 1, sib, j):
            copy.start()
        compute(0, (d, sib), j)

    def second_half(j):
        pass_far(j)
        pl.when(core == 0)(lambda: own_store(2, j).wait())
        for copy in chunk_loads(1, 0, far, j):
            copy.start()
        for a in range(2):
            for owner in (j * INNER + y, j * INNER + 1 - y):
                await_sib(a, 1, far_sib, owner)
        for copy in chunk_loads(1, 1, far_sib, j):
            copy.start()
        compute(1, (far, far_sib), j)

    def arrive(s, j):
        line_copy(s, j, True, False).wait_recv()
        relay(s, j, False, lambda copy: copy.start())
        emit(s, j)

    def take_last(r):
        pl.when(core == 0)(lambda: each(r, lambda j: take_side(2, j)))
        pl.when(core == 1)(lambda: each(r, lambda j: take_side(1, j)))

    def outward(r, carry):
        ready = line_step(z, length, r - 1)
        each(r, lambda j: arrive(0, j))
        take_last(r - 1)
        first_half(ready)
        each(r, lambda j: arrive(1, j))
        each(r, lambda j: take_side(0, j))
        second_half(ready)

        @pl.when(core == 0)
        def _():
            each(r, lambda j: arrive(2, j))
            each(r, lambda j: take_side(1, j))

        return carry

    take_side(0, z)
    pl.when(core == 0)(lambda: take_side(1, z))
    lax.fori_loop(1, length, outward, 0)
    take_last(length - 1)
    final = line_step(z, length, length - 1)
    first_half(final)
    second_half(final)
    for half, rows in enumerate(((d, sib), (far, far_sib))):
        for copy in chunk_stores(half, rows, z):
            copy.wait()
    for a in range(2):
        relay(a, z, True, lambda copy: copy.wait_send())

    def drain(j, carry):
        for s in range(3):

            def settle(s=s):
                a, row, _ = streams[s]
                if s < 2:
                    pl.when(j != z)(lambda: relay(s, j, False, lambda copy: copy.wait_send()))
                else:
                    relay(s, j, False, lambda copy: copy.wait_send())
                side_copy(s, j, True).wait_send()
                for owner in (j * INNER + y, j * INNER + 1 - y):
                    near_copies(s, place(a, row, owner), owner, lambda copy: copy.wait_send())

            on_core(s, settle)
        for owner in (j * INNER + y, j * INNER + 1 - y):
            sib_copy(0, owner).wait_send()
            pl.when(core == 1)(lambda owner=owner: sib_copy(1, owner).wait_send())
        return carry

    lax.fori_loop(0, length, drain, 0)
    pl.when(core == 0)(lambda: cross.wait_send())

    def meta_finish(i, carry):
        spread_copy(n_dp, n_ctx, i, meta_src, meta_all, meta_send, meta_recv, True).wait_send()
        return carry

    lax.fori_loop(1, n, meta_finish, 0)


def dispatch_rows(rows, grad, meta, gate_weight, up_weight, down_weight, cap, n_dp, n_ctx):
    n = n_dp * n_ctx
    length = n_ctx // INNER
    tokens, width = rows.shape
    local, _, hidden = gate_weight.shape
    low = rows.dtype
    span = 2 * INNER * cap
    arrived = jax.ShapeDtypeStruct((local, n * cap, width), low)
    dma = pltpu.SemaphoreType.DMA
    return pl.pallas_call(
        functools.partial(dispatch_kernel, n_dp, n_ctx, cap),
        out_shape=(
            arrived,
            arrived,
            jax.ShapeDtypeStruct((local, n * cap, 2 * hidden), low),
            jax.ShapeDtypeStruct((local, n * cap, hidden), low),
            arrived,
            jax.ShapeDtypeStruct((n,) + meta.shape[1:], jnp.float32),
            jax.ShapeDtypeStruct((n,) + meta.shape[1:], jnp.float32),
        ),
        in_specs=[ANY, ANY, VMEM, ANY, ANY, ANY],
        out_specs=(ANY,) * 5 + (VMEM,) * 2,
        scratch_shapes=[
            pltpu.VMEM((3, length, tokens, width), low),
            pltpu.VMEM((3, length, local, cap, width), low),
            pltpu.VMEM((3, length, local, cap, width), low),
            pltpu.VMEM((local, width, 2 * hidden), low),
            pltpu.VMEM(down_weight.shape, low),
            pltpu.VMEM((2, 2, local, span, width), low),
            pltpu.VMEM((2, local, span, 2 * hidden), low),
            pltpu.VMEM((2, local, span, hidden), low),
            pltpu.VMEM((2, local, span, width), low),
            dma((n,)),
            dma((n,)),
            dma((2,)),
            dma((3,)),
            dma((3, 2, length)),
            dma((3, length)),
            dma((3, length)),
            dma((3, length)),
            dma((2, n_ctx)),
            dma((2, n_ctx)),
            dma((2, 2, n_ctx)),
            dma((2, 2, n_ctx)),
            dma((3, length)),
            dma((2, 2, 2)),
            dma((2, 3, 2)),
            dma,
            dma,
        ],
        compiler_params=pltpu.CompilerParams(
            collective_id=0, has_side_effects=True, vmem_limit_bytes=60 * 1024 * 1024
        ),
    )(rows, grad, meta, gate_weight, up_weight, down_weight)


def return_kernel(
    n_dp, n_ctx, cap, tile, back_ref, rows_ref, grad_ref, pair_ref, hid_ref, score_ref, meta_ref,
    gate_out, up_out, down_out, out_score, out_tok,
    mine, sib_land, far_land, side_land, running, land, pair, hid_raw, hid, row_tile, grad_tile,
    both, down, mine_sem, sib_send, sib_recv, far_send, far_recv, side_send, side_recv,
    line_send, line_recv, hold_sem, tile_sem, result_sem, score_send, score_recv,
):
    d, c = lax.axis_index("dp"), lax.axis_index("ctx")
    z, y, length = line_of(c, n_ctx)
    local = back_ref.shape[0]
    picks = meta_ref.shape[1] // 2
    width, depth = rows_ref.shape[2], hid_ref.shape[2]
    across = width // tile
    units = local * across
    side = z * INNER + 1 - y
    far = lax.rem(d + 2, n_dp)
    sib = d + 1 - 2 * lax.rem(d, 2)
    far_sib = lax.rem(sib + 2, n_dp)
    greet_all(n_dp, n_ctx)

    def block(slot):
        return back_ref.at[:, pl.ds(pl.multiple_of(slot * cap, 8), cap)]

    def to_sib(owner, which):
        row = far_sib if which == 0 else sib
        return pltpu.make_async_remote_copy(
            src_ref=block(row * n_ctx + owner),
            dst_ref=sib_land.at[owner, which],
            send_sem=sib_send.at[owner, which],
            recv_sem=sib_recv.at[owner, which],
            device_id=(sib, c),
            device_id_type=MESH,
        )

    def load(owner, which):
        row = far if which == 0 else d
        return pltpu.make_async_copy(
            block(row * n_ctx + owner), mine.at[owner, which], mine_sem.at[owner, which]
        )

    def to_far(owner):
        return pltpu.make_async_remote_copy(
            src_ref=mine.at[owner, 0],
            dst_ref=far_land.at[owner],
            send_sem=far_send.at[owner],
            recv_sem=far_recv.at[owner],
            device_id=(far, c),
            device_id_type=MESH,
        )

    def to_side(j):
        return pltpu.make_async_remote_copy(
            src_ref=mine.at[j * INNER + 1 - y, 1],
            dst_ref=side_land.at[j],
            send_sem=side_send.at[j],
            recv_sem=side_recv.at[j],
            device_id=(d, side),
            device_id_type=MESH,
        )

    def along(j, up, slot):
        return pltpu.make_async_remote_copy(
            src_ref=running.at[j],
            dst_ref=land.at[slot],
            send_sem=line_send.at[j],
            recv_sem=line_recv.at[slot],
            device_id=(d, (z + (1 if up else -1)) * INNER + y),
            device_id_type=MESH,
        )

    def pass_on(j, act):
        pl.when(j > z)(lambda: act(along(j, True, j)))
        pl.when((j < z) & (j < z - 1))(lambda: act(along(j, False, j)))
        pl.when((j < z) & (j == z - 1))(lambda: act(along(j, False, length)))

    def each(r, act):
        for k in range(2):
            j = z + (2 * k - 1) * r
            pl.when((j >= 0) & (j < length) & (r + k > 0))(lambda j=j: act(j))

    def outermost(act):
        def step(i, carry):
            each(length - 1 - i, act)
            return carry

        lax.fori_loop(0, length, step, 0)

    def tile_loads(u):
        e, slot = lax.div(u, across), lax.rem(u, 2)
        columns = pl.ds(pl.multiple_of(lax.rem(u, across) * tile, tile), tile)
        return (
            pltpu.make_async_copy(
                rows_ref.at[e, :, columns], row_tile.at[slot], tile_sem.at[0, slot]
            ),
            pltpu.make_async_copy(
                grad_ref.at[e, :, columns], grad_tile.at[slot], tile_sem.at[1, slot]
            ),
        )

    def results(u):
        e = lax.div(u, across)
        columns = pl.ds(pl.multiple_of(lax.rem(u, across) * tile, tile), tile)
        return (
            pltpu.make_async_copy(
                both.at[u, :, pl.ds(0, depth)], gate_out.at[e, columns], result_sem.at[0, u]
            ),
            pltpu.make_async_copy(
                both.at[u, :, pl.ds(depth, depth)], up_out.at[e, columns], result_sem.at[1, u]
            ),
            pltpu.make_async_copy(down.at[u], down_out.at[e, :, columns], result_sem.at[2, u]),
        )

    def unit(u, carry):
        for copy in tile_loads(u):
            copy.wait()

        @pl.when(u + 1 < units)
        def _():
            for copy in tile_loads(u + 1):
                copy.start()

        e, slot = lax.div(u, across), lax.rem(u, 2)
        both[u] = jnp.dot(
            row_tile[slot].T, pair[e], preferred_element_type=jnp.float32
        ).astype(jnp.bfloat16)
        down[u] = jnp.dot(
            hid[e], grad_tile[slot], preferred_element_type=jnp.float32
        ).astype(jnp.bfloat16)
        for copy in results(u):
            copy.start()
        return carry

    n = n_dp * n_ctx
    me = d * n_ctx + c
    score_src = lambda peer: score_ref.at[peer]

    def score_start(i, carry):
        spread_copy(n_dp, n_ctx, i, score_src, out_score, score_send, score_recv, True).start()
        return carry

    def score_finish(i, carry):
        spread_copy(n_dp, n_ctx, i, score_src, out_score, score_send, score_recv, True).wait_send()
        spread_copy(n_dp, n_ctx, i, score_src, out_score, score_send, score_recv, False).wait_recv()
        return carry

    def begin(j, which):
        for at in range(INNER):
            to_sib(j * INNER + at, which).start()
            load(j * INNER + at, which).start()

    for which in range(2):
        outermost(lambda j, which=which: begin(j, which))
    holds = (
        pltpu.make_async_copy(pair_ref, pair, hold_sem.at[0]),
        pltpu.make_async_copy(hid_ref, hid_raw, hold_sem.at[1]),
    )
    for copy in holds:
        copy.start()
    for copy in tile_loads(0):
        copy.start()

    def widen(value):
        return value.astype(jnp.float32)

    def outward(j):
        for owner in (j * INNER + 1 - y, j * INNER + y):
            to_sib(owner, 0).wait_recv()
            load(owner, 0).wait()
            mine[owner, 0] = (widen(mine[owner, 0]) + widen(sib_land[owner, 0])).astype(
                jnp.bfloat16
            )
            to_far(owner).start()

    outermost(outward)
    lax.fori_loop(1, n, score_start, 0)
    out_score[pl.ds(me, 1)] = score_ref[pl.ds(me, 1)]
    for copy in holds:
        copy.wait()
    for e in range(local):
        hid[e] = hid_raw[e].T

    def inward(j):
        for owner in (j * INNER + 1 - y, j * INNER + y):
            to_sib(owner, 1).wait_recv()
            load(owner, 1).wait()
            to_far(owner).wait_recv()
            mine[owner, 1] = (
                widen(mine[owner, 1]) + widen(sib_land[owner, 1]) + widen(far_land[owner])
            ).astype(jnp.bfloat16)
        to_side(j).start()

    def spread(j):
        to_side(j).wait_recv()
        meta = meta_ref[d * n_ctx + j * INNER + y]
        total = jnp.zeros((meta.shape[1], width), jnp.float32)
        for e in range(local):
            for owner, held in (
                (c, mine[j * INNER + y, 1, e]), (side, side_land[j, e])
            ):
                masks = slot_masks(meta, picks, cap, (owner * local + e) * cap)
                pick = sum(jnp.where(mask, 1.0, 0.0) for mask in masks)
                total = total + jnp.dot(
                    pick.T.astype(jnp.bfloat16), held, preferred_element_type=jnp.float32
                )
        return total

    def combine(j):
        total = spread(j)

        def through(keep):
            running[j] = keep.astype(jnp.bfloat16)
            pass_on(j, lambda copy: copy.start())

        arrives = jnp.where(j > z, z > 0, z < length - 1)

        @pl.when(arrives)
        def _():
            along(j, True, j).wait_recv()
            through(total + widen(land[j]))

        @pl.when(jnp.logical_not(arrives))
        def _():
            through(total)

    def finish(i):
        out_tok[...] = spread(z)
        for slot, there in ((z, z > 0), (length, z < length - 1)):

            @pl.when(there)
            def _(slot=slot):
                along(z, True, slot).wait_recv()
                out_tok[...] = out_tok[...] + widen(land[slot])

    def turn(i, carry):
        r = length - 1 - i
        each(r, inward)
        lax.fori_loop(lax.div(i * units, length), lax.div((i + 1) * units, length), unit, 0)
        each(r, combine)
        return carry

    lax.fori_loop(0, length - 1, turn, 0)
    inward(z)
    lax.fori_loop(lax.div((length - 1) * units, length), units, unit, 0)
    finish(0)
    lax.fori_loop(1, n, score_finish, 0)

    def drain(j):
        for owner in (j * INNER + 1 - y, j * INNER + y):
            to_sib(owner, 0).wait_send()
            to_sib(owner, 1).wait_send()
            to_far(owner).wait_send()
        to_side(j).wait_send()
        pass_on(j, lambda copy: copy.wait_send())

    outermost(drain)

    def store_wait(u, carry):
        for copy in results(u):
            copy.wait()
        return carry

    lax.fori_loop(0, units, store_wait, 0)


def return_rows(back, rows, grad, pair, hidden, score, meta, n_dp, n_ctx):
    local, total, width = back.shape
    n = n_dp * n_ctx
    cap = total // n
    length = n_ctx // INNER
    tokens = meta.shape[2]
    depth = hidden.shape[2]
    tile = 256 if width % 256 == 0 else 128
    units = local * (width // tile)
    block = (local, cap, width)
    low = back.dtype
    dma = pltpu.SemaphoreType.DMA
    return pl.pallas_call(
        functools.partial(return_kernel, n_dp, n_ctx, cap, tile),
        out_shape=(
            jax.ShapeDtypeStruct((local, width, depth), low),
            jax.ShapeDtypeStruct((local, width, depth), low),
            jax.ShapeDtypeStruct((local, depth, width), low),
            jax.ShapeDtypeStruct(score.shape, jnp.float32),
            jax.ShapeDtypeStruct((tokens, width), jnp.float32),
        ),
        in_specs=[ANY] * 5 + [VMEM] * 2,
        out_specs=(ANY,) * 3 + (VMEM,) * 2,
        scratch_shapes=[
            pltpu.VMEM((n_ctx, 2) + block, low),
            pltpu.VMEM((n_ctx, 2) + block, low),
            pltpu.VMEM((n_ctx,) + block, low),
            pltpu.VMEM((length,) + block, low),
            pltpu.VMEM((length, tokens, width), low),
            pltpu.VMEM((length + 1, tokens, width), low),
            pltpu.VMEM((local, total, 2 * depth), low),
            pltpu.VMEM((local, total, depth), low),
            pltpu.VMEM((local, depth, total), low),
            pltpu.VMEM((2, total, tile), low),
            pltpu.VMEM((2, total, tile), low),
            pltpu.VMEM((units, tile, 2 * depth), low),
            pltpu.VMEM((units, depth, tile), low),
            dma((n_ctx, 2)),
            dma((n_ctx, 2)),
            dma((n_ctx, 2)),
            dma((n_ctx,)),
            dma((n_ctx,)),
            dma((length,)),
            dma((length,)),
            dma((length,)),
            dma((length + 1,)),
            dma((2,)),
            dma((2, 2)),
            dma((3, units)),
            dma((n,)),
            dma((n,)),
        ],
        compiler_params=pltpu.CompilerParams(
            collective_id=1, has_side_effects=True, vmem_limit_bytes=63 * 1024 * 1024
        ),
    )(back, rows, grad, pair, hidden, score, meta)


def tiles(x):
    return jnp.pad(x, ((0, 0), (0, 1024 - x.shape[1]))).reshape(x.shape[0], 8, 128)


def body(
    tokens, cotangent, expert_ids, norm_gain, router_weight, gate_weight, up_weight, down_weight
):
    n_ctx = lax.axis_size("ctx")
    n_dp = lax.axis_size("dp")
    n = n_dp * n_ctx
    local = gate_weight.shape[0]
    experts = router_weight.shape[1]
    rows_here = tokens.shape[0]
    picks = expert_ids.shape[1]
    width = tokens.shape[1]
    capacity = max(2, rows_here * picks * 5 // (4 * experts))
    capacity = -(-capacity // 8) * 8
    widened = tokens.astype(jnp.float32)
    inverse = lax.rsqrt(jnp.mean(widened * widened, axis=1, keepdims=True) + EPSILON)
    scaled = widened * inverse
    normed = (scaled * norm_gain).astype(jnp.bfloat16)
    logits = jnp.dot(normed, router_weight, preferred_element_type=jnp.float32)
    labels = jnp.arange(experts, dtype=jnp.int32)
    member = expert_ids[:, :, None] == labels
    chosen = jnp.sum(jnp.where(member, logits[:, None, :], 0.0), axis=2)
    lifted = jnp.exp(chosen)
    gates = lifted / jnp.sum(lifted, axis=1, keepdims=True)
    hits = jnp.any(member, axis=1).astype(jnp.bfloat16)
    earlier = jnp.tril(jnp.ones((rows_here, rows_here), jnp.bfloat16), -1)
    count = jnp.dot(earlier, hits, preferred_element_type=jnp.float32)
    rank = jnp.sum(jnp.where(member, count[:, None, :], 0.0), axis=2)
    position = expert_ids.astype(jnp.float32) * capacity + rank
    meta = jnp.concatenate([position, gates], axis=1).T[None]
    rows, upstream, pair, hidden, back, score, metas = dispatch_rows(
        normed, cotangent, meta, gate_weight, up_weight, down_weight, capacity, n_dp, n_ctx
    )
    gate_grad, up_grad, down_grad, score_parts, grad_tok = return_rows(
        back, rows, upstream, pair, hidden, score, metas, n_dp, n_ctx
    )
    score_tok = jnp.sum(score_parts, axis=0)[:picks].T
    mixed = jnp.sum(gates * score_tok, axis=1, keepdims=True)
    grad_chosen = gates * (score_tok - mixed)
    grad_logits = jnp.sum(jnp.where(member, grad_chosen[:, :, None], 0.0), axis=1).astype(
        jnp.bfloat16
    )
    grad_normed = grad_tok + jnp.dot(
        grad_logits, router_weight.T, preferred_element_type=jnp.float32
    )
    router_part = jnp.dot(normed.T, grad_logits, preferred_element_type=jnp.float32)
    gain_part = jnp.sum(grad_normed * scaled, axis=0)
    share = width // n
    parts = jnp.concatenate(
        [router_part.reshape(n, share * experts), gain_part.reshape(n, share)], axis=1
    )
    sums = exchange(tiles(parts), n_dp, n_ctx, 1, 3).reshape(1024)
    router_grad = sums[: share * experts].reshape(share, experts)
    gain_grad = sums[share * experts : share * experts + share]
    grad_scaled = grad_normed * norm_gain
    correction = jnp.mean(grad_scaled * scaled, axis=1, keepdims=True)
    grad_input = (
        cotangent.astype(jnp.float32) + inverse * (grad_scaled - scaled * correction)
    ).astype(jnp.bfloat16)
    return (grad_input, gate_grad, up_grad, down_grad, router_grad, gain_grad)


def solution(mesh):
    return jax.shard_map(
        body,
        mesh=mesh,
        in_specs=(
            P(("dp", "ctx"), None),
            P(("dp", "ctx"), None),
            P(("dp", "ctx"), None),
            P(),
            P(),
            P("ctx", None, "dp"),
            P("ctx", None, "dp"),
            P("ctx", "dp", None),
        ),
        out_specs=(
            P(("dp", "ctx"), None),
            P("ctx", None, "dp"),
            P("ctx", None, "dp"),
            P("ctx", "dp", None),
            P(("dp", "ctx"), None),
            P(("dp", "ctx")),
        ),
        check_vma=False,
    )
```

```python
import functools

import jax
import jax.numpy as jnp
from jax import lax
from jax.experimental import pallas as pl
from jax.experimental.pallas import tpu as pltpu
from jax.sharding import PartitionSpec as P

EPSILON = 1e-05
SWISH_SCALE = 1.702
INNER = 2
MESH = pl.DeviceIdType.MESH
ANY = pl.BlockSpec(memory_space=pl.ANY)
VMEM = pl.BlockSpec(memory_space=pltpu.VMEM)


def greet_all(n_dp, n_ctx):
    n = n_dp * n_ctx
    me = lax.axis_index("dp") * n_ctx + lax.axis_index("ctx")
    barrier = pltpu.get_barrier_semaphore()

    def hello(i, carry):
        peer = lax.rem(me + i, n)
        pl.semaphore_signal(
            barrier,
            inc=1,
            device_id=(lax.div(peer, n_ctx), lax.rem(peer, n_ctx)),
            device_id_type=MESH,
        )
        return carry

    lax.fori_loop(1, n, hello, 0)
    pl.semaphore_wait(barrier, n - 1)


def spread_copy(n_dp, n_ctx, i, src_of, land, send_sem, recv_sem, sending):
    n = n_dp * n_ctx
    me = lax.axis_index("dp") * n_ctx + lax.axis_index("ctx")
    peer = lax.rem(me + i, n)
    source = me if sending else lax.rem(me + n - i, n)
    return pltpu.make_async_remote_copy(
        src_ref=src_of(peer),
        dst_ref=land.at[source],
        send_sem=send_sem.at[i],
        recv_sem=recv_sem.at[i],
        device_id=(lax.div(peer, n_ctx), lax.rem(peer, n_ctx)),
        device_id_type=MESH,
    )


def exchange_kernel(n_dp, n_ctx, keep, x_ref, o_ref, land, send_sem, recv_sem):
    n = n_dp * n_ctx
    me = lax.axis_index("dp") * n_ctx + lax.axis_index("ctx")
    greet_all(n_dp, n_ctx)
    src_of = lambda peer: x_ref.at[peer]

    def start(i, carry):
        spread_copy(n_dp, n_ctx, i, src_of, land, send_sem, recv_sem, True).start()
        return carry

    lax.fori_loop(1, n, start, 0)
    land[pl.ds(me, 1)] = x_ref[pl.ds(me, 1)]

    def finish(i, carry):
        spread_copy(n_dp, n_ctx, i, src_of, land, send_sem, recv_sem, True).wait_send()
        spread_copy(n_dp, n_ctx, i, src_of, land, send_sem, recv_sem, False).wait_recv()
        return carry

    lax.fori_loop(1, n, finish, 0)
    o_ref[...] = jnp.sum(land[...].reshape(n // keep, keep, 8, 128), axis=0)


def exchange(x, n_dp, n_ctx, keep, cid):
    n = n_dp * n_ctx
    return pl.pallas_call(
        functools.partial(exchange_kernel, n_dp, n_ctx, keep),
        out_shape=jax.ShapeDtypeStruct((keep, 8, 128), jnp.float32),
        in_specs=[VMEM],
        out_specs=VMEM,
        scratch_shapes=[
            pltpu.VMEM((n, 8, 128), jnp.float32),
            pltpu.SemaphoreType.DMA((n,)),
            pltpu.SemaphoreType.DMA((n,)),
        ],
        compiler_params=pltpu.CompilerParams(collective_id=cid, has_side_effects=True),
    )(x)


def line_of(c, n_ctx):
    return lax.div(c, INNER), lax.rem(c, INNER), n_ctx // INNER


def line_step(z, length, q):
    near = jnp.minimum(z, length - 1 - z)
    around = z + lax.div(q + 1, 2) * (1 - 2 * lax.rem(q, 2))
    beyond = jnp.where(z < length - 1 - z, q, length - 1 - q)
    return jnp.where(q <= 2 * near, around, beyond)


def slot_masks(meta, picks, cap, base):
    places = (lax.broadcasted_iota(jnp.int32, (cap, meta.shape[1]), 0) + base).astype(jnp.float32)
    return [meta[k : k + 1] == places for k in range(picks)]


def dispatch_kernel(
    n_dp, n_ctx, cap, rows_ref, grad_ref, meta_ref, wg_ref, wu_ref, wd_ref,
    out_rows, out_grad, out_pair, out_hid, out_back, out_score, meta_all,
    dense, sel_own, sel_side, pair_w, down_w, chunk, pair_out, hid_out, back_out,
    meta_send, meta_recv, own_sem, weight_sem, line_send, line_recv, side_send, side_recv,
    far_send, far_recv, sib_send, sib_recv, store_sem, chunk_sem, result_sem,
    cross_send, cross_recv,
):
    n = n_dp * n_ctx
    local, depth = wd_ref.shape[0], wd_ref.shape[1]
    picks = meta_ref.shape[1] // 2
    d, c = lax.axis_index("dp"), lax.axis_index("ctx")
    z, y, length = line_of(c, n_ctx)
    me = d * n_ctx + c
    side = z * INNER + 1 - y
    far = lax.rem(d + 2, n_dp)
    sib = d + 1 - 2 * lax.rem(d, 2)
    far_sib = lax.rem(sib + 2, n_dp)
    core = lax.rem(d, 2)
    streams = ((0, d, 0), (1, d, 0), (1, far, 1))
    ins, outs = (rows_ref, grad_ref), (out_rows, out_grad)
    span = INNER * cap
    greet_all(n_dp, n_ctx)
    meta_src = lambda peer: meta_ref.at[0]

    def line_copy(a, j, up, first):
        return pltpu.make_async_remote_copy(
            src_ref=ins[a] if first else dense.at[a, j],
            dst_ref=dense.at[a, j],
            send_sem=line_send.at[a, int(up), j],
            recv_sem=line_recv.at[a, j],
            device_id=(d, (z + (1 if up else -1)) * INNER + y),
            device_id_type=MESH,
        )

    def relay(a, j, first, act):
        @pl.when((j <= z) & (z < length - 1))
        def _():
            act(line_copy(a, j, True, first))

        @pl.when((j >= z) & (z > 0))
        def _():
            act(line_copy(a, j, False, first))

    def meta_start(i, carry):
        spread_copy(n_dp, n_ctx, i, meta_src, meta_all, meta_send, meta_recv, True).start()
        return carry

    def on_core(s, act):
        if s == 2:
            pl.when(core == 0)(act)
        else:
            act()

    cross = pltpu.make_async_remote_copy(
        src_ref=grad_ref,
        dst_ref=dense.at[2, z],
        send_sem=cross_send,
        recv_sem=cross_recv,
        device_id=(far, c),
        device_id_type=MESH,
    )
    lax.fori_loop(1, n, meta_start, 0)
    pl.when(core == 0)(lambda: cross.start())
    for a in range(2):
        relay(a, z, True, lambda copy: copy.start())
    meta_all[pl.ds(me, 1)] = meta_ref[...]
    loads = [pltpu.make_async_copy(ins[a], dense.at[a, z], own_sem.at[a]) for a in range(2)]
    for load in loads:
        load.start()
    wloads = (
        pltpu.make_async_copy(wg_ref, pair_w.at[:, :, pl.ds(0, depth)], weight_sem.at[0]),
        pltpu.make_async_copy(wu_ref, pair_w.at[:, :, pl.ds(depth, depth)], weight_sem.at[1]),
        pltpu.make_async_copy(wd_ref, down_w, weight_sem.at[2]),
    )
    for load in wloads:
        load.start()

    def place(a, row, owner):
        slot = row * n_ctx + owner
        return outs[a].at[:, pl.ds(pl.multiple_of(slot * cap, 8), cap)]

    def forward(a, src, row, owner, to, send_sem, recv_sem):
        return pltpu.make_async_remote_copy(
            src_ref=src,
            dst_ref=place(a, row, owner),
            send_sem=send_sem,
            recv_sem=recv_sem,
            device_id=(to, c),
            device_id_type=MESH,
        )

    def near_copies(s, src, owner, act):
        a, row, which = streams[s]
        to_far = lambda: act(
            forward(a, src, row, owner, far, far_send.at[a, owner], far_recv.at[a, owner])
        )
        if s == 0:
            to_far()
        if s == 1:
            pl.when(core == 1)(to_far)
        send, recv = sib_send.at[a, which, owner], sib_recv.at[a, which, owner]
        act(forward(a, src, row, owner, sib, send, recv))

    def sib_copy(a, owner):
        src = place(a, far, owner)
        return forward(a, src, far, owner, sib, sib_send.at[a, 1, owner], sib_recv.at[a, 1, owner])

    def await_far(a, owner):
        row = place(a, far, owner)
        forward(a, row, far, owner, far, far_send.at[a, owner], far_recv.at[a, owner]).wait_recv()

    def await_sib(a, which, row, owner):
        src = place(a, row, owner)
        forward(
            a, src, row, owner, sib, sib_send.at[a, which, owner], sib_recv.at[a, which, owner]
        ).wait_recv()

    def side_copy(s, j, sending):
        a, row, _ = streams[s]
        return pltpu.make_async_remote_copy(
            src_ref=sel_side.at[s, j],
            dst_ref=place(a, row, j * INNER + (y if sending else 1 - y)),
            send_sem=side_send.at[s, j],
            recv_sem=side_recv.at[s, j],
            device_id=(d, side),
            device_id_type=MESH,
        )

    def own_store(s, j):
        a, row, _ = streams[s]
        return pltpu.make_async_copy(
            sel_own.at[s, j], place(a, row, j * INNER + y), store_sem.at[s, j]
        )

    def select(s, j):
        meta = meta_all[streams[s][1] * n_ctx + j * INNER + y]
        held = dense[s, j]
        for target, owner in ((sel_own, c), (sel_side, side)):
            for e in range(local):
                masks = slot_masks(meta, picks, cap, (owner * local + e) * cap)
                pick = sum(jnp.where(mask, 1.0, 0.0) for mask in masks).astype(jnp.bfloat16)
                target[s, j, e] = jnp.dot(
                    pick, held, preferred_element_type=jnp.float32
                ).astype(jnp.bfloat16)

    def emit(s, j):
        select(s, j)
        side_copy(s, j, True).start()
        near_copies(s, sel_own.at[s, j], j * INNER + y, lambda copy: copy.start())
        own_store(s, j).start()

    def take_side(s, j):
        side_copy(s, j, False).wait_recv()
        a, row, _ = streams[s]
        owner = j * INNER + 1 - y
        near_copies(s, place(a, row, owner), owner, lambda copy: copy.start())

    def segment(row, j):
        return pl.ds(pl.multiple_of((row * n_ctx + j * INNER) * cap, 8), span)

    def chunk_loads(half, i, row, j):
        return [
            pltpu.make_async_copy(
                outs[a].at[:, segment(row, j)],
                chunk.at[half, a, :, pl.ds(i * span, span)],
                chunk_sem.at[half, a, i],
            )
            for a in range(2)
        ]

    def chunk_stores(half, rows, j):
        return [
            pltpu.make_async_copy(
                held.at[half, :, pl.ds(i * span, span)],
                out.at[:, segment(row, j)],
                result_sem.at[half, b, i],
            )
            for b, (held, out) in enumerate(
                ((pair_out, out_pair), (hid_out, out_hid), (back_out, out_back))
            )
            for i, row in enumerate(rows)
        ]

    def compute(half, rows, j):
        for i, row in enumerate(rows):
            for copy in chunk_loads(half, i, row, j):
                copy.wait()

        @pl.when(j != z)
        def _():
            for copy in chunk_stores(half, rows, j):
                copy.wait()

        sources = [row * n_ctx + j * INNER + side_at for row in rows for side_at in range(INNER)]

        def expert(e, carry):
            masks = [
                slot_masks(meta_all[src], picks, cap, (c * local + e) * cap) for src in sources
            ]
            weight = jnp.concatenate(
                [
                    jnp.sum(
                        sum(
                            jnp.where(mask, meta_all[src, picks + k][None, :], 0.0)
                            for k, mask in enumerate(block)
                        ),
                        axis=1,
                        keepdims=True,
                    )
                    for src, block in zip(sources, masks)
                ],
                axis=0,
            )
            pre = jnp.dot(chunk[half, 0, e], pair_w[e], preferred_element_type=jnp.float32)
            grad_out = lax.dot_general(
                chunk[half, 1, e], down_w[e], (((1,), (1,)), ((), ())),
                preferred_element_type=jnp.float32,
            )
            gate_pre, up_pre = pre[:, :depth], pre[:, depth:]
            squash = jax.nn.sigmoid(SWISH_SCALE * gate_pre)
            swish = gate_pre * squash
            raised = up_pre + 1.0
            full = swish * raised
            hid_out[half, e] = (weight * full).astype(jnp.bfloat16)
            score = jnp.sum(
                grad_out * full.astype(jnp.bfloat16).astype(jnp.float32), axis=1, keepdims=True
            )
            grad_hidden = weight * grad_out
            slope = squash + SWISH_SCALE * swish * (1.0 - squash)
            pair_out[half, e, :, pl.ds(0, depth)] = (grad_hidden * raised * slope).astype(jnp.bfloat16)
            pair_out[half, e, :, pl.ds(depth, depth)] = (grad_hidden * swish).astype(jnp.bfloat16)
            back_out[half, e] = lax.dot_general(
                pair_out[half, e], pair_w[e], (((1,), (1,)), ((), ())),
                preferred_element_type=jnp.float32,
            ).astype(jnp.bfloat16)
            for i, (src, block) in enumerate(zip(sources, masks)):
                part = score[i * cap : (i + 1) * cap]
                lines = [
                    jnp.sum(jnp.where(mask, part, 0.0), axis=0, keepdims=True) for mask in block
                ]
                lines.append(jnp.zeros((picks, lines[0].shape[1]), jnp.float32))
                out_score[src] = out_score[src] + jnp.concatenate(lines, axis=0)
            return carry

        lax.fori_loop(0, local, expert, 0)
        for copy in chunk_stores(half, rows, j):
            copy.start()

    out_score[...] = jnp.zeros_like(out_score)
    for load in loads:
        load.wait()
    for a in range(2):
        emit(a, z)
    for load in wloads:
        load.wait()

    def meta_arrival(i, carry):
        spread_copy(n_dp, n_ctx, i, meta_src, meta_all, meta_send, meta_recv, False).wait_recv()
        return carry

    lax.fori_loop(1, n, meta_arrival, 0)

    @pl.when(core == 0)
    def _():
        cross.wait_recv()
        relay(2, z, False, lambda copy: copy.start())
        emit(2, z)

    def each(r, act):
        def step(k, carry):
            j = z + (2 * k - 1) * r
            pl.when((j >= 0) & (j < length) & (r + k > 0))(lambda: act(j))
            return carry

        lax.fori_loop(0, 2, step, 0)

    def pass_far(j):
        def one(a):
            for owner in (j * INNER + y, j * INNER + 1 - y):
                await_far(a, owner)
                sib_copy(a, owner).start()

        one(0)
        pl.when(core == 1)(lambda: one(1))

    def first_half(j):
        for a in range(2):
            own_store(a, j).wait()
        for copy in chunk_loads(0, 0, d, j):
            copy.start()
        for a in range(2):
            for side_at in range(INNER):
                await_sib(a, 0, sib, j * INNER + side_at)
        for copy in chunk_loads(0, 1, sib, j):
            copy.start()
        compute(0, (d, sib), j)

    def second_half(j):
        pass_far(j)
        pl.when(core == 0)(lambda: own_store(2, j).wait())
        for copy in chunk_loads(1, 0, far, j):
            copy.start()
        for a in range(2):
            for owner in (j * INNER + y, j * INNER + 1 - y):
                await_sib(a, 1, far_sib, owner)
        for copy in chunk_loads(1, 1, far_sib, j):
            copy.start()
        compute(1, (far, far_sib), j)

    def arrive(s, j):
        line_copy(s, j, True, False).wait_recv()
        relay(s, j, False, lambda copy: copy.start())
        emit(s, j)

    def take_last(r):
        pl.when(core == 0)(lambda: each(r, lambda j: take_side(2, j)))
        pl.when(core == 1)(lambda: each(r, lambda j: take_side(1, j)))

    def outward(r, carry):
        ready = line_step(z, length, r - 1)
        each(r, lambda j: arrive(0, j))
        take_last(r - 1)
        first_half(ready)
        each(r, lambda j: arrive(1, j))
        each(r, lambda j: take_side(0, j))
        second_half(ready)

        @pl.when(core == 0)
        def _():
            each(r, lambda j: arrive(2, j))
            each(r, lambda j: take_side(1, j))

        return carry

    take_side(0, z)
    pl.when(core == 0)(lambda: take_side(1, z))
    lax.fori_loop(1, length, outward, 0)
    take_last(length - 1)
    final = line_step(z, length, length - 1)
    first_half(final)
    second_half(final)
    for half, rows in enumerate(((d, sib), (far, far_sib))):
        for copy in chunk_stores(half, rows, z):
            copy.wait()
    for a in range(2):
        relay(a, z, True, lambda copy: copy.wait_send())

    def drain(j, carry):
        for s in range(3):

            def settle(s=s):
                a, row, _ = streams[s]
                if s < 2:
                    pl.when(j != z)(lambda: relay(s, j, False, lambda copy: copy.wait_send()))
                else:
                    relay(s, j, False, lambda copy: copy.wait_send())
                side_copy(s, j, True).wait_send()
                for owner in (j * INNER + y, j * INNER + 1 - y):
                    near_copies(s, place(a, row, owner), owner, lambda copy: copy.wait_send())

            on_core(s, settle)
        for owner in (j * INNER + y, j * INNER + 1 - y):
            sib_copy(0, owner).wait_send()
            pl.when(core == 1)(lambda owner=owner: sib_copy(1, owner).wait_send())
        return carry

    lax.fori_loop(0, length, drain, 0)
    pl.when(core == 0)(lambda: cross.wait_send())

    def meta_finish(i, carry):
        spread_copy(n_dp, n_ctx, i, meta_src, meta_all, meta_send, meta_recv, True).wait_send()
        return carry

    lax.fori_loop(1, n, meta_finish, 0)


def dispatch_rows(rows, grad, meta, gate_weight, up_weight, down_weight, cap, n_dp, n_ctx):
    n = n_dp * n_ctx
    length = n_ctx // INNER
    tokens, width = rows.shape
    local, _, hidden = gate_weight.shape
    low = rows.dtype
    span = 2 * INNER * cap
    arrived = jax.ShapeDtypeStruct((local, n * cap, width), low)
    dma = pltpu.SemaphoreType.DMA
    return pl.pallas_call(
        functools.partial(dispatch_kernel, n_dp, n_ctx, cap),
        out_shape=(
            arrived,
            arrived,
            jax.ShapeDtypeStruct((local, n * cap, 2 * hidden), low),
            jax.ShapeDtypeStruct((local, n * cap, hidden), low),
            arrived,
            jax.ShapeDtypeStruct((n,) + meta.shape[1:], jnp.float32),
            jax.ShapeDtypeStruct((n,) + meta.shape[1:], jnp.float32),
        ),
        in_specs=[ANY, ANY, VMEM, ANY, ANY, ANY],
        out_specs=(ANY,) * 5 + (VMEM,) * 2,
        scratch_shapes=[
            pltpu.VMEM((3, length, tokens, width), low),
            pltpu.VMEM((3, length, local, cap, width), low),
            pltpu.VMEM((3, length, local, cap, width), low),
            pltpu.VMEM((local, width, 2 * hidden), low),
            pltpu.VMEM(down_weight.shape, low),
            pltpu.VMEM((2, 2, local, span, width), low),
            pltpu.VMEM((2, local, span, 2 * hidden), low),
            pltpu.VMEM((2, local, span, hidden), low),
            pltpu.VMEM((2, local, span, width), low),
            dma((n,)),
            dma((n,)),
            dma((2,)),
            dma((3,)),
            dma((3, 2, length)),
            dma((3, length)),
            dma((3, length)),
            dma((3, length)),
            dma((2, n_ctx)),
            dma((2, n_ctx)),
            dma((2, 2, n_ctx)),
            dma((2, 2, n_ctx)),
            dma((3, length)),
            dma((2, 2, 2)),
            dma((2, 3, 2)),
            dma,
            dma,
        ],
        compiler_params=pltpu.CompilerParams(
            collective_id=0, has_side_effects=True, vmem_limit_bytes=60 * 1024 * 1024
        ),
    )(rows, grad, meta, gate_weight, up_weight, down_weight)


def return_kernel(
    n_dp, n_ctx, cap, tile, back_ref, rows_ref, grad_ref, pair_ref, hid_ref, score_ref, meta_ref,
    gate_out, up_out, down_out, out_score, out_tok,
    mine, sib_land, far_land, side_land, running, land, pair, hid_raw, hid, row_tile, grad_tile,
    both, down, mine_sem, sib_send, sib_recv, far_send, far_recv, side_send, side_recv,
    line_send, line_recv, hold_sem, tile_sem, result_sem, score_send, score_recv,
):
    d, c = lax.axis_index("dp"), lax.axis_index("ctx")
    z, y, length = line_of(c, n_ctx)
    local = back_ref.shape[0]
    picks = meta_ref.shape[1] // 2
    width, depth = rows_ref.shape[2], hid_ref.shape[2]
    across = width // tile
    units = local * across
    side = z * INNER + 1 - y
    far = lax.rem(d + 2, n_dp)
    sib = d + 1 - 2 * lax.rem(d, 2)
    far_sib = lax.rem(sib + 2, n_dp)
    greet_all(n_dp, n_ctx)

    def block(slot):
        return back_ref.at[:, pl.ds(pl.multiple_of(slot * cap, 8), cap)]

    def to_sib(owner, which):
        row = far_sib if which == 0 else sib
        return pltpu.make_async_remote_copy(
            src_ref=block(row * n_ctx + owner),
            dst_ref=sib_land.at[owner, which],
            send_sem=sib_send.at[owner, which],
            recv_sem=sib_recv.at[owner, which],
            device_id=(sib, c),
            device_id_type=MESH,
        )

    def load(owner, which):
        row = far if which == 0 else d
        return pltpu.make_async_copy(
            block(row * n_ctx + owner), mine.at[owner, which], mine_sem.at[owner, which]
        )

    def to_far(owner):
        return pltpu.make_async_remote_copy(
            src_ref=mine.at[owner, 0],
            dst_ref=far_land.at[owner],
            send_sem=far_send.at[owner],
            recv_sem=far_recv.at[owner],
            device_id=(far, c),
            device_id_type=MESH,
        )

    def to_side(j):
        return pltpu.make_async_remote_copy(
            src_ref=mine.at[j * INNER + 1 - y, 1],
            dst_ref=side_land.at[j],
            send_sem=side_send.at[j],
            recv_sem=side_recv.at[j],
            device_id=(d, side),
            device_id_type=MESH,
        )

    def along(j, up, slot):
        return pltpu.make_async_remote_copy(
            src_ref=running.at[j],
            dst_ref=land.at[slot],
            send_sem=line_send.at[j],
            recv_sem=line_recv.at[slot],
            device_id=(d, (z + (1 if up else -1)) * INNER + y),
            device_id_type=MESH,
        )

    def pass_on(j, act):
        pl.when(j > z)(lambda: act(along(j, True, j)))
        pl.when((j < z) & (j < z - 1))(lambda: act(along(j, False, j)))
        pl.when((j < z) & (j == z - 1))(lambda: act(along(j, False, length)))

    def each(r, act):
        for k in range(2):
            j = z + (2 * k - 1) * r
            pl.when((j >= 0) & (j < length) & (r + k > 0))(lambda j=j: act(j))

    def outermost(act):
        def step(i, carry):
            each(length - 1 - i, act)
            return carry

        lax.fori_loop(0, length, step, 0)

    def tile_loads(u):
        e, slot = lax.div(u, across), lax.rem(u, 2)
        columns = pl.ds(pl.multiple_of(lax.rem(u, across) * tile, tile), tile)
        return (
            pltpu.make_async_copy(
                rows_ref.at[e, :, columns], row_tile.at[slot], tile_sem.at[0, slot]
            ),
            pltpu.make_async_copy(
                grad_ref.at[e, :, columns], grad_tile.at[slot], tile_sem.at[1, slot]
            ),
        )

    def results(u):
        e = lax.div(u, across)
        columns = pl.ds(pl.multiple_of(lax.rem(u, across) * tile, tile), tile)
        return (
            pltpu.make_async_copy(
                both.at[u, :, pl.ds(0, depth)], gate_out.at[e, columns], result_sem.at[0, u]
            ),
            pltpu.make_async_copy(
                both.at[u, :, pl.ds(depth, depth)], up_out.at[e, columns], result_sem.at[1, u]
            ),
            pltpu.make_async_copy(down.at[u], down_out.at[e, :, columns], result_sem.at[2, u]),
        )

    def unit(u, carry):
        for copy in tile_loads(u):
            copy.wait()

        @pl.when(u + 1 < units)
        def _():
            for copy in tile_loads(u + 1):
                copy.start()

        e, slot = lax.div(u, across), lax.rem(u, 2)
        both[u] = jnp.dot(
            row_tile[slot].T, pair[e], preferred_element_type=jnp.float32
        ).astype(jnp.bfloat16)
        down[u] = jnp.dot(
            hid[e], grad_tile[slot], preferred_element_type=jnp.float32
        ).astype(jnp.bfloat16)
        for copy in results(u):
            copy.start()
        return carry

    n = n_dp * n_ctx
    me = d * n_ctx + c
    score_src = lambda peer: score_ref.at[peer]

    def score_start(i, carry):
        spread_copy(n_dp, n_ctx, i, score_src, out_score, score_send, score_recv, True).start()
        return carry

    def score_finish(i, carry):
        spread_copy(n_dp, n_ctx, i, score_src, out_score, score_send, score_recv, True).wait_send()
        spread_copy(n_dp, n_ctx, i, score_src, out_score, score_send, score_recv, False).wait_recv()
        return carry

    def begin(j, which):
        for at in range(INNER):
            to_sib(j * INNER + at, which).start()
            load(j * INNER + at, which).start()

    for which in range(2):
        outermost(lambda j, which=which: begin(j, which))
    holds = (
        pltpu.make_async_copy(pair_ref, pair, hold_sem.at[0]),
        pltpu.make_async_copy(hid_ref, hid_raw, hold_sem.at[1]),
    )
    for copy in holds:
        copy.start()
    for copy in tile_loads(0):
        copy.start()

    def widen(value):
        return value.astype(jnp.float32)

    def outward(j):
        for owner in (j * INNER + 1 - y, j * INNER + y):
            to_sib(owner, 0).wait_recv()
            load(owner, 0).wait()
            mine[owner, 0] = (widen(mine[owner, 0]) + widen(sib_land[owner, 0])).astype(
                jnp.bfloat16
            )
            to_far(owner).start()

    outermost(outward)
    lax.fori_loop(1, n, score_start, 0)
    out_score[pl.ds(me, 1)] = score_ref[pl.ds(me, 1)]
    for copy in holds:
        copy.wait()
    for e in range(local):
        hid[e] = hid_raw[e].T

    def inward(j):
        theirs = j * INNER + 1 - y
        for owner in (theirs, j * INNER + y):
            to_sib(owner, 1).wait_recv()
            load(owner, 1).wait()
            to_far(owner).wait_recv()
            mine[owner, 1] = (
                widen(mine[owner, 1]) + widen(sib_land[owner, 1]) + widen(far_land[owner])
            ).astype(jnp.bfloat16)
            if owner is theirs:
                to_side(j).start()

    def spread(j):
        to_side(j).wait_recv()
        meta = meta_ref[d * n_ctx + j * INNER + y]
        total = jnp.zeros((meta.shape[1], width), jnp.float32)
        for e in range(local):
            for owner, held in (
                (c, mine[j * INNER + y, 1, e]), (side, side_land[j, e])
            ):
                masks = slot_masks(meta, picks, cap, (owner * local + e) * cap)
                pick = sum(jnp.where(mask, 1.0, 0.0) for mask in masks)
                total = total + jnp.dot(
                    pick.T.astype(jnp.bfloat16), held, preferred_element_type=jnp.float32
                )
        return total

    def combine(j):
        total = spread(j)

        def through(keep):
            running[j] = keep.astype(jnp.bfloat16)
            pass_on(j, lambda copy: copy.start())

        arrives = jnp.where(j > z, z > 0, z < length - 1)

        @pl.when(arrives)
        def _():
            along(j, True, j).wait_recv()
            through(total + widen(land[j]))

        @pl.when(jnp.logical_not(arrives))
        def _():
            through(total)

    def finish(i):
        out_tok[...] = spread(z)
        for slot, there in ((z, z > 0), (length, z < length - 1)):

            @pl.when(there)
            def _(slot=slot):
                along(z, True, slot).wait_recv()
                out_tok[...] = out_tok[...] + widen(land[slot])

    def turn(i, carry):
        r = length - 1 - i
        each(r, inward)
        lax.fori_loop(lax.div(i * units, length), lax.div((i + 1) * units, length), unit, 0)
        each(r, combine)
        return carry

    lax.fori_loop(0, length - 1, turn, 0)
    inward(z)
    lax.fori_loop(lax.div((length - 1) * units, length), units, unit, 0)
    finish(0)
    lax.fori_loop(1, n, score_finish, 0)

    def drain(j):
        for owner in (j * INNER + 1 - y, j * INNER + y):
            to_sib(owner, 0).wait_send()
            to_sib(owner, 1).wait_send()
            to_far(owner).wait_send()
        to_side(j).wait_send()
        pass_on(j, lambda copy: copy.wait_send())

    outermost(drain)

    def store_wait(u, carry):
        for copy in results(u):
            copy.wait()
        return carry

    lax.fori_loop(0, units, store_wait, 0)


def return_rows(back, rows, grad, pair, hidden, score, meta, n_dp, n_ctx):
    local, total, width = back.shape
    n = n_dp * n_ctx
    cap = total // n
    length = n_ctx // INNER
    tokens = meta.shape[2]
    depth = hidden.shape[2]
    tile = 256 if width % 256 == 0 else 128
    units = local * (width // tile)
    block = (local, cap, width)
    low = back.dtype
    dma = pltpu.SemaphoreType.DMA
    return pl.pallas_call(
        functools.partial(return_kernel, n_dp, n_ctx, cap, tile),
        out_shape=(
            jax.ShapeDtypeStruct((local, width, depth), low),
            jax.ShapeDtypeStruct((local, width, depth), low),
            jax.ShapeDtypeStruct((local, depth, width), low),
            jax.ShapeDtypeStruct(score.shape, jnp.float32),
            jax.ShapeDtypeStruct((tokens, width), jnp.float32),
        ),
        in_specs=[ANY] * 5 + [VMEM] * 2,
        out_specs=(ANY,) * 3 + (VMEM,) * 2,
        scratch_shapes=[
            pltpu.VMEM((n_ctx, 2) + block, low),
            pltpu.VMEM((n_ctx, 2) + block, low),
            pltpu.VMEM((n_ctx,) + block, low),
            pltpu.VMEM((length,) + block, low),
            pltpu.VMEM((length, tokens, width), low),
            pltpu.VMEM((length + 1, tokens, width), low),
            pltpu.VMEM((local, total, 2 * depth), low),
            pltpu.VMEM((local, total, depth), low),
            pltpu.VMEM((local, depth, total), low),
            pltpu.VMEM((2, total, tile), low),
            pltpu.VMEM((2, total, tile), low),
            pltpu.VMEM((units, tile, 2 * depth), low),
            pltpu.VMEM((units, depth, tile), low),
            dma((n_ctx, 2)),
            dma((n_ctx, 2)),
            dma((n_ctx, 2)),
            dma((n_ctx,)),
            dma((n_ctx,)),
            dma((length,)),
            dma((length,)),
            dma((length,)),
            dma((length + 1,)),
            dma((2,)),
            dma((2, 2)),
            dma((3, units)),
            dma((n,)),
            dma((n,)),
        ],
        compiler_params=pltpu.CompilerParams(
            collective_id=1, has_side_effects=True, vmem_limit_bytes=63 * 1024 * 1024
        ),
    )(back, rows, grad, pair, hidden, score, meta)


def finish_kernel(
    tok_ref, cot_ref, norm_ref, gain_ref, router_ref, ids_ref, meta_ref, score_ref, grad_ref,
    gate_ref, up_ref, down_ref, out_tok, sums, gate_out, up_out, down_out,
    gate_held, up_held, down_held, load_sem, store_sem,
):
    local, picks = gate_ref.shape[0], ids_ref.shape[0]
    experts = router_ref.shape[0]
    moved = ((gate_ref, gate_held, gate_out), (up_ref, up_held, up_out))
    moved = moved + ((down_ref, down_held, down_out),)
    loads = [
        pltpu.make_async_copy(src.at[e], held.at[e], load_sem.at[i, e])
        for i, (src, held, _) in enumerate(moved)
        for e in range(local)
    ]
    stores = [
        pltpu.make_async_copy(held.at[e], out.at[e], store_sem.at[i, e])
        for i, (_, held, out) in enumerate(moved)
        for e in range(local)
    ]
    for load in loads:
        load.start()
    score = jnp.sum(score_ref[...], axis=0)[:picks]
    gates = meta_ref[picks : 2 * picks]
    mixed = jnp.sum(gates * score, axis=0, keepdims=True)
    grad_chosen = gates * (score - mixed)
    labels = lax.broadcasted_iota(jnp.int32, (experts, score.shape[1]), 0)
    grad_logits = sum(
        jnp.where(ids_ref[k : k + 1] == labels, grad_chosen[k : k + 1], 0.0) for k in range(picks)
    )
    sums[:experts] = jnp.dot(
        grad_logits.astype(jnp.bfloat16), norm_ref[...], preferred_element_type=jnp.float32
    )
    for load, store in zip(loads, stores):
        load.wait()
        store.start()
    grad_normed = grad_ref[...] + jnp.dot(
        grad_logits.T.astype(jnp.bfloat16), router_ref[...], preferred_element_type=jnp.float32
    )
    widened = tok_ref[...].astype(jnp.float32)
    inverse = lax.rsqrt(jnp.mean(widened * widened, axis=1, keepdims=True) + EPSILON)
    scaled = widened * inverse
    gained = jnp.sum(grad_normed * scaled, axis=0, keepdims=True)
    sums[experts:] = jnp.broadcast_to(gained, (8, gained.shape[1]))
    grad_scaled = grad_normed * gain_ref[...]
    correction = jnp.mean(grad_scaled * scaled, axis=1, keepdims=True)
    out_tok[...] = (
        cot_ref[...].astype(jnp.float32) + inverse * (grad_scaled - scaled * correction)
    ).astype(jnp.bfloat16)
    for store in stores:
        store.wait()


def finish_rows(values, weights):
    tokens, router = values[0], values[4]
    dma = pltpu.SemaphoreType.DMA
    return pl.pallas_call(
        finish_kernel,
        out_shape=(
            jax.ShapeDtypeStruct(tokens.shape, tokens.dtype),
            jax.ShapeDtypeStruct((router.shape[0] + 8, router.shape[1]), jnp.float32),
        )
        + tuple(jax.ShapeDtypeStruct(weight.shape, weight.dtype) for weight in weights),
        in_specs=[VMEM] * len(values) + [ANY] * 3,
        out_specs=(VMEM, VMEM) + (ANY,) * 3,
        scratch_shapes=[pltpu.VMEM(weight.shape, weight.dtype) for weight in weights]
        + [dma((3, weights[0].shape[0]))] * 2,
        compiler_params=pltpu.CompilerParams(vmem_limit_bytes=60 * 1024 * 1024),
    )(*values, *weights)


def tiles(x):
    return jnp.pad(x, ((0, 0), (0, 1024 - x.shape[1]))).reshape(x.shape[0], 8, 128)


def body(
    tokens, cotangent, expert_ids, norm_gain, router_weight, gate_weight, up_weight, down_weight
):
    n_ctx = lax.axis_size("ctx")
    n_dp = lax.axis_size("dp")
    n = n_dp * n_ctx
    local = gate_weight.shape[0]
    experts = router_weight.shape[1]
    rows_here = tokens.shape[0]
    picks = expert_ids.shape[1]
    width = tokens.shape[1]
    capacity = max(2, rows_here * picks * 5 // (4 * experts))
    capacity = -(-capacity // 8) * 8
    widened = tokens.astype(jnp.float32)
    inverse = lax.rsqrt(jnp.mean(widened * widened, axis=1, keepdims=True) + EPSILON)
    scaled = widened * inverse
    normed = (scaled * norm_gain).astype(jnp.bfloat16)
    logits = jnp.dot(normed, router_weight, preferred_element_type=jnp.float32)
    labels = jnp.arange(experts, dtype=jnp.int32)
    member = expert_ids[:, :, None] == labels
    chosen = jnp.sum(jnp.where(member, logits[:, None, :], 0.0), axis=2)
    lifted = jnp.exp(chosen)
    gates = lifted / jnp.sum(lifted, axis=1, keepdims=True)
    hits = jnp.any(member, axis=1).astype(jnp.bfloat16)
    earlier = jnp.tril(jnp.ones((rows_here, rows_here), jnp.bfloat16), -1)
    count = jnp.dot(earlier, hits, preferred_element_type=jnp.float32)
    rank = jnp.sum(jnp.where(member, count[:, None, :], 0.0), axis=2)
    position = expert_ids.astype(jnp.float32) * capacity + rank
    meta = jnp.concatenate([position, gates], axis=1).T[None]
    rows, upstream, pair, hidden, back, score, metas = dispatch_rows(
        normed, cotangent, meta, gate_weight, up_weight, down_weight, capacity, n_dp, n_ctx
    )
    gate_grad, up_grad, down_grad, score_parts, grad_tok = return_rows(
        back, rows, upstream, pair, hidden, score, metas, n_dp, n_ctx
    )
    values = (tokens, cotangent, normed, norm_gain[None], router_weight.T, expert_ids.T)
    grad_input, total, gate_grad, up_grad, down_grad = finish_rows(
        values + (meta[0], score_parts, grad_tok), (gate_grad, up_grad, down_grad)
    )
    router_part, gain_part = total[:experts].T, total[experts]
    share = width // n
    parts = jnp.concatenate(
        [router_part.reshape(n, share * experts), gain_part.reshape(n, share)], axis=1
    )
    sums = exchange(tiles(parts), n_dp, n_ctx, 1, 3).reshape(1024)
    router_grad = sums[: share * experts].reshape(share, experts)
    gain_grad = sums[share * experts : share * experts + share]
    return (grad_input, gate_grad, up_grad, down_grad, router_grad, gain_grad)


def solution(mesh):
    return jax.shard_map(
        body,
        mesh=mesh,
        in_specs=(
            P(("dp", "ctx"), None),
            P(("dp", "ctx"), None),
            P(("dp", "ctx"), None),
            P(),
            P(),
            P("ctx", None, "dp"),
            P("ctx", None, "dp"),
            P("ctx", "dp", None),
        ),
        out_specs=(
            P(("dp", "ctx"), None),
            P("ctx", None, "dp"),
            P("ctx", None, "dp"),
            P("ctx", "dp", None),
            P(("dp", "ctx"), None),
            P(("dp", "ctx")),
        ),
        check_vma=False,
    )
```

```python
import functools

import jax
import jax.numpy as jnp
from jax import lax
from jax.experimental import pallas as pl
from jax.experimental.pallas import tpu as pltpu
from jax.sharding import PartitionSpec as P

EPSILON = 1e-05
SWISH_SCALE = 1.702
INNER = 2
MESH = pl.DeviceIdType.MESH
ANY = pl.BlockSpec(memory_space=pl.ANY)
VMEM = pl.BlockSpec(memory_space=pltpu.VMEM)


def greet_all(n_dp, n_ctx):
    n = n_dp * n_ctx
    me = lax.axis_index("dp") * n_ctx + lax.axis_index("ctx")
    barrier = pltpu.get_barrier_semaphore()

    def hello(i, carry):
        peer = lax.rem(me + i, n)
        pl.semaphore_signal(
            barrier,
            inc=1,
            device_id=(lax.div(peer, n_ctx), lax.rem(peer, n_ctx)),
            device_id_type=MESH,
        )
        return carry

    lax.fori_loop(1, n, hello, 0)
    pl.semaphore_wait(barrier, n - 1)


def spread_copy(n_dp, n_ctx, i, src_of, land, send_sem, recv_sem, sending):
    n = n_dp * n_ctx
    me = lax.axis_index("dp") * n_ctx + lax.axis_index("ctx")
    peer = lax.rem(me + i, n)
    source = me if sending else lax.rem(me + n - i, n)
    return pltpu.make_async_remote_copy(
        src_ref=src_of(peer),
        dst_ref=land.at[source],
        send_sem=send_sem.at[i],
        recv_sem=recv_sem.at[i],
        device_id=(lax.div(peer, n_ctx), lax.rem(peer, n_ctx)),
        device_id_type=MESH,
    )


def exchange_kernel(n_dp, n_ctx, keep, x_ref, o_ref, land, send_sem, recv_sem):
    n = n_dp * n_ctx
    me = lax.axis_index("dp") * n_ctx + lax.axis_index("ctx")
    greet_all(n_dp, n_ctx)
    src_of = lambda peer: x_ref.at[peer]

    def start(i, carry):
        spread_copy(n_dp, n_ctx, i, src_of, land, send_sem, recv_sem, True).start()
        return carry

    lax.fori_loop(1, n, start, 0)
    land[pl.ds(me, 1)] = x_ref[pl.ds(me, 1)]

    def finish(i, carry):
        spread_copy(n_dp, n_ctx, i, src_of, land, send_sem, recv_sem, True).wait_send()
        spread_copy(n_dp, n_ctx, i, src_of, land, send_sem, recv_sem, False).wait_recv()
        return carry

    lax.fori_loop(1, n, finish, 0)
    o_ref[...] = jnp.sum(land[...].reshape(n // keep, keep, 8, 128), axis=0)


def exchange(x, n_dp, n_ctx, keep, cid):
    n = n_dp * n_ctx
    return pl.pallas_call(
        functools.partial(exchange_kernel, n_dp, n_ctx, keep),
        out_shape=jax.ShapeDtypeStruct((keep, 8, 128), jnp.float32),
        in_specs=[VMEM],
        out_specs=VMEM,
        scratch_shapes=[
            pltpu.VMEM((n, 8, 128), jnp.float32),
            pltpu.SemaphoreType.DMA((n,)),
            pltpu.SemaphoreType.DMA((n,)),
        ],
        compiler_params=pltpu.CompilerParams(collective_id=cid, has_side_effects=True),
    )(x)


def line_of(c, n_ctx):
    return lax.div(c, INNER), lax.rem(c, INNER), n_ctx // INNER


def line_step(z, length, q):
    near = jnp.minimum(z, length - 1 - z)
    around = z + lax.div(q + 1, 2) * (1 - 2 * lax.rem(q, 2))
    beyond = jnp.where(z < length - 1 - z, q, length - 1 - q)
    return jnp.where(q <= 2 * near, around, beyond)


def slot_masks(meta, picks, cap, base):
    places = (lax.broadcasted_iota(jnp.int32, (cap, meta.shape[1]), 0) + base).astype(jnp.float32)
    return [meta[k : k + 1] == places for k in range(picks)]


def dispatch_kernel(
    n_dp, n_ctx, cap, rows_ref, grad_ref, meta_ref, wg_ref, wu_ref, wd_ref,
    out_rows, out_grad, out_pair, out_hid, out_back, out_score, meta_all,
    dense, sel_own, sel_side, pair_w, down_w, chunk, pair_out, hid_out, back_out,
    meta_send, meta_recv, own_sem, weight_sem, line_send, line_recv, side_send, side_recv,
    far_send, far_recv, sib_send, sib_recv, store_sem, chunk_sem, result_sem,
    cross_send, cross_recv,
):
    n = n_dp * n_ctx
    local, depth = wd_ref.shape[0], wd_ref.shape[1]
    picks = meta_ref.shape[1] // 2
    d, c = lax.axis_index("dp"), lax.axis_index("ctx")
    z, y, length = line_of(c, n_ctx)
    me = d * n_ctx + c
    side = z * INNER + 1 - y
    far = lax.rem(d + 2, n_dp)
    sib = d + 1 - 2 * lax.rem(d, 2)
    far_sib = lax.rem(sib + 2, n_dp)
    core = lax.rem(d, 2)
    streams = ((0, d, 0), (1, d, 0), (1, far, 1))
    ins, outs = (rows_ref, grad_ref), (out_rows, out_grad)
    span = INNER * cap
    greet_all(n_dp, n_ctx)
    meta_src = lambda peer: meta_ref.at[0]

    def line_copy(a, j, up, first):
        return pltpu.make_async_remote_copy(
            src_ref=ins[a] if first else dense.at[a, j],
            dst_ref=dense.at[a, j],
            send_sem=line_send.at[a, int(up), j],
            recv_sem=line_recv.at[a, j],
            device_id=(d, (z + (1 if up else -1)) * INNER + y),
            device_id_type=MESH,
        )

    def relay(a, j, first, act):
        @pl.when((j <= z) & (z < length - 1))
        def _():
            act(line_copy(a, j, True, first))

        @pl.when((j >= z) & (z > 0))
        def _():
            act(line_copy(a, j, False, first))

    def meta_start(i, carry):
        spread_copy(n_dp, n_ctx, i, meta_src, meta_all, meta_send, meta_recv, True).start()
        return carry

    def on_core(s, act):
        if s == 2:
            pl.when(core == 0)(act)
        else:
            act()

    cross = pltpu.make_async_remote_copy(
        src_ref=grad_ref,
        dst_ref=dense.at[2, z],
        send_sem=cross_send,
        recv_sem=cross_recv,
        device_id=(far, c),
        device_id_type=MESH,
    )
    lax.fori_loop(1, n, meta_start, 0)
    pl.when(core == 0)(lambda: cross.start())
    for a in range(2):
        relay(a, z, True, lambda copy: copy.start())
    meta_all[pl.ds(me, 1)] = meta_ref[...]
    loads = [pltpu.make_async_copy(ins[a], dense.at[a, z], own_sem.at[a]) for a in range(2)]
    for load in loads:
        load.start()
    wloads = (
        pltpu.make_async_copy(wg_ref, pair_w.at[:, :, pl.ds(0, depth)], weight_sem.at[0]),
        pltpu.make_async_copy(wu_ref, pair_w.at[:, :, pl.ds(depth, depth)], weight_sem.at[1]),
        pltpu.make_async_copy(wd_ref, down_w, weight_sem.at[2]),
    )
    for load in wloads:
        load.start()

    def place(a, row, owner):
        slot = row * n_ctx + owner
        return outs[a].at[:, pl.ds(pl.multiple_of(slot * cap, 8), cap)]

    def forward(a, src, row, owner, to, send_sem, recv_sem):
        return pltpu.make_async_remote_copy(
            src_ref=src,
            dst_ref=place(a, row, owner),
            send_sem=send_sem,
            recv_sem=recv_sem,
            device_id=(to, c),
            device_id_type=MESH,
        )

    def near_copies(s, src, owner, act):
        a, row, which = streams[s]
        to_far = lambda: act(
            forward(a, src, row, owner, far, far_send.at[a, owner], far_recv.at[a, owner])
        )
        if s == 0:
            to_far()
        if s == 1:
            pl.when(core == 1)(to_far)
        send, recv = sib_send.at[a, which, owner], sib_recv.at[a, which, owner]
        act(forward(a, src, row, owner, sib, send, recv))

    def sib_copy(a, owner):
        src = place(a, far, owner)
        return forward(a, src, far, owner, sib, sib_send.at[a, 1, owner], sib_recv.at[a, 1, owner])

    def await_far(a, owner):
        row = place(a, far, owner)
        forward(a, row, far, owner, far, far_send.at[a, owner], far_recv.at[a, owner]).wait_recv()

    def await_sib(a, which, row, owner):
        src = place(a, row, owner)
        forward(
            a, src, row, owner, sib, sib_send.at[a, which, owner], sib_recv.at[a, which, owner]
        ).wait_recv()

    def side_copy(s, j, sending):
        a, row, _ = streams[s]
        return pltpu.make_async_remote_copy(
            src_ref=sel_side.at[s, j],
            dst_ref=place(a, row, j * INNER + (y if sending else 1 - y)),
            send_sem=side_send.at[s, j],
            recv_sem=side_recv.at[s, j],
            device_id=(d, side),
            device_id_type=MESH,
        )

    def own_store(s, j):
        a, row, _ = streams[s]
        return pltpu.make_async_copy(
            sel_own.at[s, j], place(a, row, j * INNER + y), store_sem.at[s, j]
        )

    def select(s, j):
        meta = meta_all[streams[s][1] * n_ctx + j * INNER + y]
        held = dense[s, j]
        for target, owner in ((sel_own, c), (sel_side, side)):
            for e in range(local):
                masks = slot_masks(meta, picks, cap, (owner * local + e) * cap)
                pick = sum(jnp.where(mask, 1.0, 0.0) for mask in masks).astype(jnp.bfloat16)
                target[s, j, e] = jnp.dot(
                    pick, held, preferred_element_type=jnp.float32
                ).astype(jnp.bfloat16)

    def emit(s, j):
        select(s, j)
        side_copy(s, j, True).start()
        near_copies(s, sel_own.at[s, j], j * INNER + y, lambda copy: copy.start())
        own_store(s, j).start()

    def take_side(s, j):
        side_copy(s, j, False).wait_recv()
        a, row, _ = streams[s]
        owner = j * INNER + 1 - y
        near_copies(s, place(a, row, owner), owner, lambda copy: copy.start())

    def segment(row, j):
        return pl.ds(pl.multiple_of((row * n_ctx + j * INNER) * cap, 8), span)

    def chunk_loads(half, i, row, j):
        return [
            pltpu.make_async_copy(
                outs[a].at[:, segment(row, j)],
                chunk.at[half, a, :, pl.ds(i * span, span)],
                chunk_sem.at[half, a, i],
            )
            for a in range(2)
        ]

    def chunk_stores(half, rows, j):
        return [
            pltpu.make_async_copy(
                held.at[half, :, pl.ds(i * span, span)],
                out.at[:, segment(row, j)],
                result_sem.at[half, b, i],
            )
            for b, (held, out) in enumerate(
                ((pair_out, out_pair), (hid_out, out_hid), (back_out, out_back))
            )
            for i, row in enumerate(rows)
        ]

    def compute(half, rows, j):
        for i, row in enumerate(rows):
            for copy in chunk_loads(half, i, row, j):
                copy.wait()

        @pl.when(j != z)
        def _():
            for copy in chunk_stores(half, rows, j):
                copy.wait()

        sources = [row * n_ctx + j * INNER + side_at for row in rows for side_at in range(INNER)]

        def expert(e, carry):
            masks = [
                slot_masks(meta_all[src], picks, cap, (c * local + e) * cap) for src in sources
            ]
            weight = jnp.concatenate(
                [
                    jnp.sum(
                        sum(
                            jnp.where(mask, meta_all[src, picks + k][None, :], 0.0)
                            for k, mask in enumerate(block)
                        ),
                        axis=1,
                        keepdims=True,
                    )
                    for src, block in zip(sources, masks)
                ],
                axis=0,
            )
            pre = jnp.dot(chunk[half, 0, e], pair_w[e], preferred_element_type=jnp.float32)
            grad_out = lax.dot_general(
                chunk[half, 1, e], down_w[e], (((1,), (1,)), ((), ())),
                preferred_element_type=jnp.float32,
            )
            gate_pre, up_pre = pre[:, :depth], pre[:, depth:]
            squash = jax.nn.sigmoid(SWISH_SCALE * gate_pre)
            swish = gate_pre * squash
            raised = up_pre + 1.0
            full = swish * raised
            hid_out[half, e] = (weight * full).astype(jnp.bfloat16)
            score = jnp.sum(
                grad_out * full.astype(jnp.bfloat16).astype(jnp.float32), axis=1, keepdims=True
            )
            grad_hidden = weight * grad_out
            slope = squash + SWISH_SCALE * swish * (1.0 - squash)
            pair_out[half, e, :, pl.ds(0, depth)] = (grad_hidden * raised * slope).astype(jnp.bfloat16)
            pair_out[half, e, :, pl.ds(depth, depth)] = (grad_hidden * swish).astype(jnp.bfloat16)
            back_out[half, e] = lax.dot_general(
                pair_out[half, e], pair_w[e], (((1,), (1,)), ((), ())),
                preferred_element_type=jnp.float32,
            ).astype(jnp.bfloat16)
            for i, (src, block) in enumerate(zip(sources, masks)):
                part = score[i * cap : (i + 1) * cap]
                lines = [
                    jnp.sum(jnp.where(mask, part, 0.0), axis=0, keepdims=True) for mask in block
                ]
                lines.append(jnp.zeros((picks, lines[0].shape[1]), jnp.float32))
                out_score[src] = out_score[src] + jnp.concatenate(lines, axis=0)
            return carry

        lax.fori_loop(0, local, expert, 0)
        for copy in chunk_stores(half, rows, j):
            copy.start()

    out_score[...] = jnp.zeros_like(out_score)
    for load in loads:
        load.wait()
    for a in range(2):
        emit(a, z)
    for load in wloads:
        load.wait()

    def meta_arrival(i, carry):
        spread_copy(n_dp, n_ctx, i, meta_src, meta_all, meta_send, meta_recv, False).wait_recv()
        return carry

    lax.fori_loop(1, n, meta_arrival, 0)

    @pl.when(core == 0)
    def _():
        cross.wait_recv()
        relay(2, z, False, lambda copy: copy.start())
        emit(2, z)

    def each(r, act):
        def step(k, carry):
            j = z + (2 * k - 1) * r
            pl.when((j >= 0) & (j < length) & (r + k > 0))(lambda: act(j))
            return carry

        lax.fori_loop(0, 2, step, 0)

    def pass_far(j):
        def one(a):
            for owner in (j * INNER + y, j * INNER + 1 - y):
                await_far(a, owner)
                sib_copy(a, owner).start()

        one(0)
        pl.when(core == 1)(lambda: one(1))

    def first_half(j):
        for a in range(2):
            own_store(a, j).wait()
        for copy in chunk_loads(0, 0, d, j):
            copy.start()
        for a in range(2):
            for side_at in range(INNER):
                await_sib(a, 0, sib, j * INNER + side_at)
        for copy in chunk_loads(0, 1, sib, j):
            copy.start()
        compute(0, (d, sib), j)

    def second_half(j):
        pass_far(j)
        pl.when(core == 0)(lambda: own_store(2, j).wait())
        for copy in chunk_loads(1, 0, far, j):
            copy.start()
        for a in range(2):
            for owner in (j * INNER + y, j * INNER + 1 - y):
                await_sib(a, 1, far_sib, owner)
        for copy in chunk_loads(1, 1, far_sib, j):
            copy.start()
        compute(1, (far, far_sib), j)

    def arrive(s, j):
        line_copy(s, j, True, False).wait_recv()
        relay(s, j, False, lambda copy: copy.start())
        emit(s, j)

    def take_last(r):
        pl.when(core == 0)(lambda: each(r, lambda j: take_side(2, j)))
        pl.when(core == 1)(lambda: each(r, lambda j: take_side(1, j)))

    def outward(r, carry):
        ready = line_step(z, length, r - 1)
        each(r, lambda j: arrive(0, j))
        take_last(r - 1)
        first_half(ready)
        each(r, lambda j: arrive(1, j))
        each(r, lambda j: take_side(0, j))

        @pl.when(core == 0)
        def _():
            each(r, lambda j: arrive(2, j))
            each(r, lambda j: take_side(1, j))

        second_half(ready)
        return carry

    take_side(0, z)
    pl.when(core == 0)(lambda: take_side(1, z))
    lax.fori_loop(1, length, outward, 0)
    take_last(length - 1)
    final = line_step(z, length, length - 1)
    first_half(final)
    second_half(final)
    for half, rows in enumerate(((d, sib), (far, far_sib))):
        for copy in chunk_stores(half, rows, z):
            copy.wait()
    for a in range(2):
        relay(a, z, True, lambda copy: copy.wait_send())

    def drain(j, carry):
        for s in range(3):

            def settle(s=s):
                a, row, _ = streams[s]
                if s < 2:
                    pl.when(j != z)(lambda: relay(s, j, False, lambda copy: copy.wait_send()))
                else:
                    relay(s, j, False, lambda copy: copy.wait_send())
                side_copy(s, j, True).wait_send()
                for owner in (j * INNER + y, j * INNER + 1 - y):
                    near_copies(s, place(a, row, owner), owner, lambda copy: copy.wait_send())

            on_core(s, settle)
        for owner in (j * INNER + y, j * INNER + 1 - y):
            sib_copy(0, owner).wait_send()
            pl.when(core == 1)(lambda owner=owner: sib_copy(1, owner).wait_send())
        return carry

    lax.fori_loop(0, length, drain, 0)
    pl.when(core == 0)(lambda: cross.wait_send())

    def meta_finish(i, carry):
        spread_copy(n_dp, n_ctx, i, meta_src, meta_all, meta_send, meta_recv, True).wait_send()
        return carry

    lax.fori_loop(1, n, meta_finish, 0)


def dispatch_rows(rows, grad, meta, gate_weight, up_weight, down_weight, cap, n_dp, n_ctx):
    n = n_dp * n_ctx
    length = n_ctx // INNER
    tokens, width = rows.shape
    local, _, hidden = gate_weight.shape
    low = rows.dtype
    span = 2 * INNER * cap
    arrived = jax.ShapeDtypeStruct((local, n * cap, width), low)
    dma = pltpu.SemaphoreType.DMA
    return pl.pallas_call(
        functools.partial(dispatch_kernel, n_dp, n_ctx, cap),
        out_shape=(
            arrived,
            arrived,
            jax.ShapeDtypeStruct((local, n * cap, 2 * hidden), low),
            jax.ShapeDtypeStruct((local, n * cap, hidden), low),
            arrived,
            jax.ShapeDtypeStruct((n,) + meta.shape[1:], jnp.float32),
            jax.ShapeDtypeStruct((n,) + meta.shape[1:], jnp.float32),
        ),
        in_specs=[ANY, ANY, VMEM, ANY, ANY, ANY],
        out_specs=(ANY,) * 5 + (VMEM,) * 2,
        scratch_shapes=[
            pltpu.VMEM((3, length, tokens, width), low),
            pltpu.VMEM((3, length, local, cap, width), low),
            pltpu.VMEM((3, length, local, cap, width), low),
            pltpu.VMEM((local, width, 2 * hidden), low),
            pltpu.VMEM(down_weight.shape, low),
            pltpu.VMEM((2, 2, local, span, width), low),
            pltpu.VMEM((2, local, span, 2 * hidden), low),
            pltpu.VMEM((2, local, span, hidden), low),
            pltpu.VMEM((2, local, span, width), low),
            dma((n,)),
            dma((n,)),
            dma((2,)),
            dma((3,)),
            dma((3, 2, length)),
            dma((3, length)),
            dma((3, length)),
            dma((3, length)),
            dma((2, n_ctx)),
            dma((2, n_ctx)),
            dma((2, 2, n_ctx)),
            dma((2, 2, n_ctx)),
            dma((3, length)),
            dma((2, 2, 2)),
            dma((2, 3, 2)),
            dma,
            dma,
        ],
        compiler_params=pltpu.CompilerParams(
            collective_id=0, has_side_effects=True, vmem_limit_bytes=60 * 1024 * 1024
        ),
    )(rows, grad, meta, gate_weight, up_weight, down_weight)


def return_kernel(
    n_dp, n_ctx, cap, tile, back_ref, rows_ref, grad_ref, pair_ref, hid_ref, score_ref, meta_ref,
    gate_out, up_out, down_out, out_score, out_tok,
    mine, sib_land, far_land, side_land, running, land, pair, hid_raw, hid, row_tile, grad_tile,
    both, down, mine_sem, sib_send, sib_recv, far_send, far_recv, side_send, side_recv,
    line_send, line_recv, hold_sem, tile_sem, result_sem, score_send, score_recv,
):
    d, c = lax.axis_index("dp"), lax.axis_index("ctx")
    z, y, length = line_of(c, n_ctx)
    local = back_ref.shape[0]
    picks = meta_ref.shape[1] // 2
    width, depth = rows_ref.shape[2], hid_ref.shape[2]
    across = width // tile
    units = local * across
    side = z * INNER + 1 - y
    far = lax.rem(d + 2, n_dp)
    sib = d + 1 - 2 * lax.rem(d, 2)
    far_sib = lax.rem(sib + 2, n_dp)
    greet_all(n_dp, n_ctx)

    def block(slot):
        return back_ref.at[:, pl.ds(pl.multiple_of(slot * cap, 8), cap)]

    def to_sib(owner, which):
        row = far_sib if which == 0 else sib
        return pltpu.make_async_remote_copy(
            src_ref=block(row * n_ctx + owner),
            dst_ref=sib_land.at[owner, which],
            send_sem=sib_send.at[owner, which],
            recv_sem=sib_recv.at[owner, which],
            device_id=(sib, c),
            device_id_type=MESH,
        )

    def load(owner, which):
        row = far if which == 0 else d
        return pltpu.make_async_copy(
            block(row * n_ctx + owner), mine.at[owner, which], mine_sem.at[owner, which]
        )

    def to_far(owner):
        return pltpu.make_async_remote_copy(
            src_ref=mine.at[owner, 0],
            dst_ref=far_land.at[owner],
            send_sem=far_send.at[owner],
            recv_sem=far_recv.at[owner],
            device_id=(far, c),
            device_id_type=MESH,
        )

    def to_side(j):
        return pltpu.make_async_remote_copy(
            src_ref=mine.at[j * INNER + 1 - y, 1],
            dst_ref=side_land.at[j],
            send_sem=side_send.at[j],
            recv_sem=side_recv.at[j],
            device_id=(d, side),
            device_id_type=MESH,
        )

    def along(j, up, slot):
        return pltpu.make_async_remote_copy(
            src_ref=running.at[j],
            dst_ref=land.at[slot],
            send_sem=line_send.at[j],
            recv_sem=line_recv.at[slot],
            device_id=(d, (z + (1 if up else -1)) * INNER + y),
            device_id_type=MESH,
        )

    def pass_on(j, act):
        pl.when(j > z)(lambda: act(along(j, True, j)))
        pl.when((j < z) & (j < z - 1))(lambda: act(along(j, False, j)))
        pl.when((j < z) & (j == z - 1))(lambda: act(along(j, False, length)))

    def each(r, act):
        for k in range(2):
            j = z + (2 * k - 1) * r
            pl.when((j >= 0) & (j < length) & (r + k > 0))(lambda j=j: act(j))

    def outermost(act):
        def step(i, carry):
            each(length - 1 - i, act)
            return carry

        lax.fori_loop(0, length, step, 0)

    def tile_loads(u):
        e, slot = lax.div(u, across), lax.rem(u, 2)
        columns = pl.ds(pl.multiple_of(lax.rem(u, across) * tile, tile), tile)
        return (
            pltpu.make_async_copy(
                rows_ref.at[e, :, columns], row_tile.at[slot], tile_sem.at[0, slot]
            ),
            pltpu.make_async_copy(
                grad_ref.at[e, :, columns], grad_tile.at[slot], tile_sem.at[1, slot]
            ),
        )

    def results(u):
        e = lax.div(u, across)
        columns = pl.ds(pl.multiple_of(lax.rem(u, across) * tile, tile), tile)
        return (
            pltpu.make_async_copy(
                both.at[u, :, pl.ds(0, depth)], gate_out.at[e, columns], result_sem.at[0, u]
            ),
            pltpu.make_async_copy(
                both.at[u, :, pl.ds(depth, depth)], up_out.at[e, columns], result_sem.at[1, u]
            ),
            pltpu.make_async_copy(down.at[u], down_out.at[e, :, columns], result_sem.at[2, u]),
        )

    def unit(u, carry):
        for copy in tile_loads(u):
            copy.wait()

        @pl.when(u + 1 < units)
        def _():
            for copy in tile_loads(u + 1):
                copy.start()

        e, slot = lax.div(u, across), lax.rem(u, 2)
        both[u] = jnp.dot(
            row_tile[slot].T, pair[e], preferred_element_type=jnp.float32
        ).astype(jnp.bfloat16)
        down[u] = jnp.dot(
            hid[e], grad_tile[slot], preferred_element_type=jnp.float32
        ).astype(jnp.bfloat16)
        for copy in results(u):
            copy.start()
        return carry

    n = n_dp * n_ctx
    me = d * n_ctx + c
    score_src = lambda peer: score_ref.at[peer]

    def score_start(i, carry):
        spread_copy(n_dp, n_ctx, i, score_src, out_score, score_send, score_recv, True).start()
        return carry

    def score_finish(i, carry):
        spread_copy(n_dp, n_ctx, i, score_src, out_score, score_send, score_recv, True).wait_send()
        spread_copy(n_dp, n_ctx, i, score_src, out_score, score_send, score_recv, False).wait_recv()
        return carry

    def begin(j, which):
        for at in range(INNER):
            to_sib(j * INNER + at, which).start()
            load(j * INNER + at, which).start()

    for which in range(2):
        outermost(lambda j, which=which: begin(j, which))
    holds = (
        pltpu.make_async_copy(pair_ref, pair, hold_sem.at[0]),
        pltpu.make_async_copy(hid_ref, hid_raw, hold_sem.at[1]),
    )
    for copy in holds:
        copy.start()
    for copy in tile_loads(0):
        copy.start()

    def widen(value):
        return value.astype(jnp.float32)

    def outward(j):
        for owner in (j * INNER + 1 - y, j * INNER + y):
            to_sib(owner, 0).wait_recv()
            load(owner, 0).wait()
            mine[owner, 0] = (widen(mine[owner, 0]) + widen(sib_land[owner, 0])).astype(
                jnp.bfloat16
            )
            to_far(owner).start()

    outermost(outward)
    lax.fori_loop(1, n, score_start, 0)
    out_score[pl.ds(me, 1)] = score_ref[pl.ds(me, 1)]
    for copy in holds:
        copy.wait()
    for e in range(local):
        hid[e] = hid_raw[e].T

    def inward(j):
        theirs = j * INNER + 1 - y
        for owner in (theirs, j * INNER + y):
            to_sib(owner, 1).wait_recv()
            load(owner, 1).wait()
            to_far(owner).wait_recv()
            mine[owner, 1] = (
                widen(mine[owner, 1]) + widen(sib_land[owner, 1]) + widen(far_land[owner])
            ).astype(jnp.bfloat16)
            if owner is theirs:
                to_side(j).start()

    def spread(j):
        to_side(j).wait_recv()
        meta = meta_ref[d * n_ctx + j * INNER + y]
        total = jnp.zeros((meta.shape[1], width), jnp.float32)
        for e in range(local):
            for owner, held in (
                (c, mine[j * INNER + y, 1, e]), (side, side_land[j, e])
            ):
                masks = slot_masks(meta, picks, cap, (owner * local + e) * cap)
                pick = sum(jnp.where(mask, 1.0, 0.0) for mask in masks)
                total = total + jnp.dot(
                    pick.T.astype(jnp.bfloat16), held, preferred_element_type=jnp.float32
                )
        return total

    def combine(j):
        total = spread(j)

        def through(keep):
            running[j] = keep.astype(jnp.bfloat16)
            pass_on(j, lambda copy: copy.start())

        arrives = jnp.where(j > z, z > 0, z < length - 1)

        @pl.when(arrives)
        def _():
            along(j, True, j).wait_recv()
            through(total + widen(land[j]))

        @pl.when(jnp.logical_not(arrives))
        def _():
            through(total)

    def finish(i):
        out_tok[...] = spread(z)
        for slot, there in ((z, z > 0), (length, z < length - 1)):

            @pl.when(there)
            def _(slot=slot):
                along(z, True, slot).wait_recv()
                out_tok[...] = out_tok[...] + widen(land[slot])

    def turn(i, carry):
        r = length - 1 - i
        each(r, inward)
        lax.fori_loop(lax.div(i * units, length), lax.div((i + 1) * units, length), unit, 0)
        each(r, combine)
        return carry

    lax.fori_loop(0, length - 1, turn, 0)
    inward(z)
    lax.fori_loop(lax.div((length - 1) * units, length), units, unit, 0)
    finish(0)
    lax.fori_loop(1, n, score_finish, 0)

    def drain(j):
        for owner in (j * INNER + 1 - y, j * INNER + y):
            to_sib(owner, 0).wait_send()
            to_sib(owner, 1).wait_send()
            to_far(owner).wait_send()
        to_side(j).wait_send()
        pass_on(j, lambda copy: copy.wait_send())

    outermost(drain)

    def store_wait(u, carry):
        for copy in results(u):
            copy.wait()
        return carry

    lax.fori_loop(0, units, store_wait, 0)


def return_rows(back, rows, grad, pair, hidden, score, meta, n_dp, n_ctx):
    local, total, width = back.shape
    n = n_dp * n_ctx
    cap = total // n
    length = n_ctx // INNER
    tokens = meta.shape[2]
    depth = hidden.shape[2]
    tile = 256 if width % 256 == 0 else 128
    units = local * (width // tile)
    block = (local, cap, width)
    low = back.dtype
    dma = pltpu.SemaphoreType.DMA
    return pl.pallas_call(
        functools.partial(return_kernel, n_dp, n_ctx, cap, tile),
        out_shape=(
            jax.ShapeDtypeStruct((local, width, depth), low),
            jax.ShapeDtypeStruct((local, width, depth), low),
            jax.ShapeDtypeStruct((local, depth, width), low),
            jax.ShapeDtypeStruct(score.shape, jnp.float32),
            jax.ShapeDtypeStruct((tokens, width), jnp.float32),
        ),
        in_specs=[ANY] * 5 + [VMEM] * 2,
        out_specs=(ANY,) * 3 + (VMEM,) * 2,
        scratch_shapes=[
            pltpu.VMEM((n_ctx, 2) + block, low),
            pltpu.VMEM((n_ctx, 2) + block, low),
            pltpu.VMEM((n_ctx,) + block, low),
            pltpu.VMEM((length,) + block, low),
            pltpu.VMEM((length, tokens, width), low),
            pltpu.VMEM((length + 1, tokens, width), low),
            pltpu.VMEM((local, total, 2 * depth), low),
            pltpu.VMEM((local, total, depth), low),
            pltpu.VMEM((local, depth, total), low),
            pltpu.VMEM((2, total, tile), low),
            pltpu.VMEM((2, total, tile), low),
            pltpu.VMEM((units, tile, 2 * depth), low),
            pltpu.VMEM((units, depth, tile), low),
            dma((n_ctx, 2)),
            dma((n_ctx, 2)),
            dma((n_ctx, 2)),
            dma((n_ctx,)),
            dma((n_ctx,)),
            dma((length,)),
            dma((length,)),
            dma((length,)),
            dma((length + 1,)),
            dma((2,)),
            dma((2, 2)),
            dma((3, units)),
            dma((n,)),
            dma((n,)),
        ],
        compiler_params=pltpu.CompilerParams(
            collective_id=1, has_side_effects=True, vmem_limit_bytes=63 * 1024 * 1024
        ),
    )(back, rows, grad, pair, hidden, score, meta)


def finish_kernel(
    tok_ref, cot_ref, norm_ref, gain_ref, router_ref, ids_ref, meta_ref, score_ref, grad_ref,
    gate_ref, up_ref, down_ref, out_tok, sums, gate_out, up_out, down_out,
    gate_held, up_held, down_held, load_sem, store_sem,
):
    local, picks = gate_ref.shape[0], ids_ref.shape[0]
    experts = router_ref.shape[0]
    moved = ((gate_ref, gate_held, gate_out), (up_ref, up_held, up_out))
    moved = moved + ((down_ref, down_held, down_out),)
    loads = [
        pltpu.make_async_copy(src.at[e], held.at[e], load_sem.at[i, e])
        for i, (src, held, _) in enumerate(moved)
        for e in range(local)
    ]
    stores = [
        pltpu.make_async_copy(held.at[e], out.at[e], store_sem.at[i, e])
        for i, (_, held, out) in enumerate(moved)
        for e in range(local)
    ]
    for load in loads:
        load.start()
    score = jnp.sum(score_ref[...], axis=0)[:picks]
    gates = meta_ref[picks : 2 * picks]
    mixed = jnp.sum(gates * score, axis=0, keepdims=True)
    grad_chosen = gates * (score - mixed)
    labels = lax.broadcasted_iota(jnp.int32, (experts, score.shape[1]), 0)
    grad_logits = sum(
        jnp.where(ids_ref[k : k + 1] == labels, grad_chosen[k : k + 1], 0.0) for k in range(picks)
    )
    sums[:experts] = jnp.dot(
        grad_logits.astype(jnp.bfloat16), norm_ref[...], preferred_element_type=jnp.float32
    )
    for load, store in zip(loads, stores):
        load.wait()
        store.start()
    grad_normed = grad_ref[...] + jnp.dot(
        grad_logits.T.astype(jnp.bfloat16), router_ref[...], preferred_element_type=jnp.float32
    )
    widened = tok_ref[...].astype(jnp.float32)
    inverse = lax.rsqrt(jnp.mean(widened * widened, axis=1, keepdims=True) + EPSILON)
    scaled = widened * inverse
    gained = jnp.sum(grad_normed * scaled, axis=0, keepdims=True)
    sums[experts:] = jnp.broadcast_to(gained, (8, gained.shape[1]))
    grad_scaled = grad_normed * gain_ref[...]
    correction = jnp.mean(grad_scaled * scaled, axis=1, keepdims=True)
    out_tok[...] = (
        cot_ref[...].astype(jnp.float32) + inverse * (grad_scaled - scaled * correction)
    ).astype(jnp.bfloat16)
    for store in stores:
        store.wait()


def finish_rows(values, weights):
    tokens, router = values[0], values[4]
    dma = pltpu.SemaphoreType.DMA
    return pl.pallas_call(
        finish_kernel,
        out_shape=(
            jax.ShapeDtypeStruct(tokens.shape, tokens.dtype),
            jax.ShapeDtypeStruct((router.shape[0] + 8, router.shape[1]), jnp.float32),
        )
        + tuple(jax.ShapeDtypeStruct(weight.shape, weight.dtype) for weight in weights),
        in_specs=[VMEM] * len(values) + [ANY] * 3,
        out_specs=(VMEM, VMEM) + (ANY,) * 3,
        scratch_shapes=[pltpu.VMEM(weight.shape, weight.dtype) for weight in weights]
        + [dma((3, weights[0].shape[0]))] * 2,
        compiler_params=pltpu.CompilerParams(vmem_limit_bytes=60 * 1024 * 1024),
    )(*values, *weights)


def tiles(x):
    return jnp.pad(x, ((0, 0), (0, 1024 - x.shape[1]))).reshape(x.shape[0], 8, 128)


def body(
    tokens, cotangent, expert_ids, norm_gain, router_weight, gate_weight, up_weight, down_weight
):
    n_ctx = lax.axis_size("ctx")
    n_dp = lax.axis_size("dp")
    n = n_dp * n_ctx
    local = gate_weight.shape[0]
    experts = router_weight.shape[1]
    rows_here = tokens.shape[0]
    picks = expert_ids.shape[1]
    width = tokens.shape[1]
    capacity = max(2, rows_here * picks * 5 // (4 * experts))
    capacity = -(-capacity // 8) * 8
    widened = tokens.astype(jnp.float32)
    inverse = lax.rsqrt(jnp.mean(widened * widened, axis=1, keepdims=True) + EPSILON)
    scaled = widened * inverse
    normed = (scaled * norm_gain).astype(jnp.bfloat16)
    logits = jnp.dot(normed, router_weight, preferred_element_type=jnp.float32)
    labels = jnp.arange(experts, dtype=jnp.int32)
    member = expert_ids[:, :, None] == labels
    chosen = jnp.sum(jnp.where(member, logits[:, None, :], 0.0), axis=2)
    lifted = jnp.exp(chosen)
    gates = lifted / jnp.sum(lifted, axis=1, keepdims=True)
    hits = jnp.any(member, axis=1).astype(jnp.bfloat16)
    earlier = jnp.tril(jnp.ones((rows_here, rows_here), jnp.bfloat16), -1)
    count = jnp.dot(earlier, hits, preferred_element_type=jnp.float32)
    rank = jnp.sum(jnp.where(member, count[:, None, :], 0.0), axis=2)
    position = expert_ids.astype(jnp.float32) * capacity + rank
    meta = jnp.concatenate([position, gates], axis=1).T[None]
    rows, upstream, pair, hidden, back, score, metas = dispatch_rows(
        normed, cotangent, meta, gate_weight, up_weight, down_weight, capacity, n_dp, n_ctx
    )
    gate_grad, up_grad, down_grad, score_parts, grad_tok = return_rows(
        back, rows, upstream, pair, hidden, score, metas, n_dp, n_ctx
    )
    values = (tokens, cotangent, normed, norm_gain[None], router_weight.T, expert_ids.T)
    grad_input, total, gate_grad, up_grad, down_grad = finish_rows(
        values + (meta[0], score_parts, grad_tok), (gate_grad, up_grad, down_grad)
    )
    router_part, gain_part = total[:experts].T, total[experts]
    share = width // n
    parts = jnp.concatenate(
        [router_part.reshape(n, share * experts), gain_part.reshape(n, share)], axis=1
    )
    sums = exchange(tiles(parts), n_dp, n_ctx, 1, 3).reshape(1024)
    router_grad = sums[: share * experts].reshape(share, experts)
    gain_grad = sums[share * experts : share * experts + share]
    return (grad_input, gate_grad, up_grad, down_grad, router_grad, gain_grad)


def solution(mesh):
    return jax.shard_map(
        body,
        mesh=mesh,
        in_specs=(
            P(("dp", "ctx"), None),
            P(("dp", "ctx"), None),
            P(("dp", "ctx"), None),
            P(),
            P(),
            P("ctx", None, "dp"),
            P("ctx", None, "dp"),
            P("ctx", "dp", None),
        ),
        out_specs=(
            P(("dp", "ctx"), None),
            P("ctx", None, "dp"),
            P("ctx", None, "dp"),
            P("ctx", "dp", None),
            P(("dp", "ctx"), None),
            P(("dp", "ctx")),
        ),
        check_vma=False,
    )
```
